256 devices in a mesh: sy: 16 (over y, z_lo), sx: 16 (over z_hi, x, core).
Axes of the slice: x: 4, y: 4, z: 8 (z_hi: 2, z_lo: 4; z = z_hi * 4 + z_lo), core: 2. Of those that a mesh axis runs over, the one named last changes fastest.
Arguments:
- object_re: float32 [4096, 4096], P('sy', 'sx'), may hold values from -6 to 6
- object_im: float32 [4096, 4096], P('sy', 'sx'), may hold values from -6 to 6
- probe_re: float32 [2, 256, 256], replicated, may hold values from -6 to 6
- probe_im: float32 [2, 256, 256], replicated, may hold values from -6 to 6
- amplitudes: float32 [16, 16, 8, 256, 256], P('sy', 'sx'), may hold values from 0.5 to 3
- offsets: int32 [16, 16, 8, 2], P('sy', 'sx'), may hold values from -128 to 127
- visit_order: int32 [16, 16, 8], P('sy', 'sx'), may hold values from 0 to 7, each once within a row
Outputs:
- object_new_re: float32 [4096, 4096], P('sy', 'sx')
- object_new_im: float32 [4096, 4096], P('sy', 'sx')
- probe_new_re: float32 [2, 256, 256], replicated
- probe_new_im: float32 [2, 256, 256], replicated
The draws below stay inside these ranges and needn't reach their ends.
Inputs may be any that keep to these rules, and one draw needn't show every extreme that they name: `visit_order`: each tile's entries are a permutation of 0 to 7.
All inputs are finite; a program needn't handle non-finite values.
Results may differ from the reference program's by a relative error of at most 0.0019.
Values sent between devices are 32-bit elements; how exact they have to be, the bound alone decides.
A program may use at most 64 MiB of HBM per device.

```python
import math
import jax
import jax.numpy as jnp
from jax import lax

FRAME = 256
MODES = 2
POS_DEV = 8
BATCHES = 2
TILE = 256
HALO = 128
TILE_ROWS = 16
TILE_COLS = 16
NY = 4096
NX = 4096
N_SY = 16
N_SX = 16


def place_ends(values, own_key, low, top_value):
    shape = values.shape
    spot = [jax.random.randint(jax.random.fold_in(own_key, axis), (), 0, shape[axis]) for axis in range(len(shape))]
    values = values.at[tuple(spot)].set(low)
    longest = shape.index(max(shape))
    spot[longest] = (spot[longest] + 1) % shape[longest]
    return values.at[tuple(spot)].set(top_value)


def levels(own_key, shape, split, low, high):
    gain, own = 1.0, jax.random.fold_in(own_key, 6)
    for dim, shards_of in split:
        heights = jnp.exp(jax.random.uniform(jax.random.fold_in(own, dim), (shards_of,), jnp.float32, low / len(split), high / len(split)))
        gain = gain * jnp.repeat(heights, shape[dim] // shards_of).reshape([-1 if axis == dim else 1 for axis in range(len(shape))])
    return gain


def noise(own_key, shape, spread, bound, shards=(), held_as=jnp.bfloat16):
    result = jax.random.normal(own_key, shape, jnp.float32) * spread
    if len(shards) > 0:
        result = levels(own_key, shape, shards, -0.22, 0.18) * result
    return jnp.clip(result, min=-bound, max=bound).astype(held_as)


def setup_inputs(seed: int = 0) -> dict:
    seeds = jax.random.split(jax.random.key(seed), 8)
    object_re = noise(seeds[0], (NY, NX), 1.0, 6.0, ((0, 16), (1, 16)), jnp.float32)
    object_im = noise(seeds[1], (NY, NX), 1.0, 6.0, ((0, 16), (1, 16)), jnp.float32)
    probe_re = noise(seeds[2], (MODES, FRAME, FRAME), 1.0, 6.0, (), jnp.float32)
    probe_im = noise(seeds[3], (MODES, FRAME, FRAME), 1.0, 6.0, (), jnp.float32)
    amplitudes = jnp.clip(0.5 + 2.5 * jax.random.uniform(seeds[4], (TILE_ROWS, TILE_COLS, POS_DEV, FRAME, FRAME), jnp.float32) ** levels(seeds[4], (TILE_ROWS, TILE_COLS, POS_DEV, FRAME, FRAME), ((0, 16), (1, 16)), -0.2, 0.2), 0.5, 3.0)
    offsets = place_ends(jax.random.randint(seeds[5], (TILE_ROWS, TILE_COLS, POS_DEV, 2), -HALO, HALO), jax.random.fold_in(seeds[5], 1), -HALO, HALO - 1).astype(jnp.int32)
    visit_order = jax.vmap(lambda own: jax.random.permutation(own, POS_DEV))(jax.random.split(seeds[6], TILE_ROWS * TILE_COLS)).reshape((TILE_ROWS, TILE_COLS, POS_DEV)).astype(jnp.int32)
    return {"object_re": object_re, "object_im": object_im, "probe_re": probe_re, "probe_im": probe_im, "amplitudes": amplitudes, "offsets": offsets, "visit_order": visit_order}


OBJECT_RATE = 0.25
PROBE_GAIN = 4.0

def dft_tables(frame_size):
    ramp_values = jnp.arange(frame_size, dtype=jnp.int32)
    product = ramp_values[:, None] * ramp_values[None, :] % frame_size
    phase_angle = 2.0 * math.pi / frame_size * product.astype(jnp.float32)
    norm_scale = 1.0 / math.sqrt(frame_size)
    table_re = (jnp.cos(phase_angle) * norm_scale).astype(jnp.bfloat16)
    table_im = (-jnp.sin(phase_angle) * norm_scale).astype(jnp.bfloat16)
    return (table_re, table_im)

def left_product(matrix, values_in):
    return jnp.einsum('jk,bmkl->bmjl', matrix.astype(jnp.float32), values_in.astype(jnp.float32))

def right_product(values_in, matrix):
    return jnp.einsum('bmjk,kl->bmjl', values_in.astype(jnp.float32), matrix.astype(jnp.float32))

def transform(real_part, imag_part, table_re, table_im):
    half_re = (left_product(table_re, real_part) - left_product(table_im, imag_part)).astype(jnp.bfloat16)
    half_im = (left_product(table_re, imag_part) + left_product(table_im, real_part)).astype(jnp.bfloat16)
    far_re = right_product(half_re, table_re) - right_product(half_im, table_im)
    far_im = right_product(half_im, table_re) + right_product(half_re, table_im)
    return (far_re, far_im)

def correct(patch_re, patch_im, chosen_amps, probe_re, probe_im, table_re, table_im):
    exit_re = (probe_re[None] * patch_re[:, None] - probe_im[None] * patch_im[:, None]).astype(jnp.bfloat16)
    exit_im = (probe_re[None] * patch_im[:, None] + probe_im[None] * patch_re[:, None]).astype(jnp.bfloat16)
    far_re, far_im = transform(exit_re, exit_im, table_re, table_im)
    intensity = lax.optimization_barrier(jnp.sum(far_re * far_re + far_im * far_im, axis=1))
    amp_ratio = chosen_amps / jnp.sqrt(jnp.maximum(intensity, 1.0))
    fixed_re = (far_re * amp_ratio[:, None]).astype(jnp.bfloat16)
    fixed_im = (far_im * amp_ratio[:, None]).astype(jnp.bfloat16)
    back_re, back_im = transform(fixed_re, fixed_im, table_re, -table_im)
    delta_re = back_re - exit_re.astype(jnp.float32)
    delta_im = back_im - exit_im.astype(jnp.float32)
    object_grad_re = lax.optimization_barrier(jnp.sum(probe_re[None] * delta_re + probe_im[None] * delta_im, axis=1))
    object_grad_im = lax.optimization_barrier(jnp.sum(probe_re[None] * delta_im - probe_im[None] * delta_re, axis=1))
    probe_grad_re = lax.optimization_barrier(jnp.sum(patch_re[:, None] * delta_re + patch_im[:, None] * delta_im, axis=0))
    probe_grad_im = lax.optimization_barrier(jnp.sum(patch_re[:, None] * delta_im - patch_im[:, None] * delta_re, axis=0))
    return (object_grad_re, object_grad_im, probe_grad_re, probe_grad_im)

def reference(object_re, object_im, probe_re, probe_im, amplitudes, offsets, visit_order):
    table_re, table_im = dft_tables(FRAME)
    tile_count = N_SY * N_SX
    batch_size = POS_DEV // BATCHES
    amp_flat = amplitudes.reshape(tile_count, POS_DEV, FRAME, FRAME)
    offset_flat = offsets.reshape(tile_count, POS_DEV, 2)
    order_flat = visit_order.reshape(tile_count, POS_DEV)
    probe_power = jnp.max(lax.optimization_barrier(jnp.sum(probe_re * probe_re + probe_im * probe_im, axis=0)))
    object_pair = jnp.pad(jnp.stack([object_re, object_im]), ((0, 0), (HALO, HALO), (HALO, HALO)))
    grad_re = jnp.zeros((MODES, FRAME, FRAME), jnp.float32)
    grad_im = jnp.zeros((MODES, FRAME, FRAME), jnp.float32)
    for batch_index in range(BATCHES):

        def one_tile(tile_index, loop_state):
            accum, probe_acc_re, probe_acc_im = loop_state
            tile_row = (tile_index // N_SX).astype(jnp.int32)
            tile_col = (tile_index % N_SX).astype(jnp.int32)
            order_row = lax.dynamic_index_in_dim(order_flat, tile_index, 0, keepdims=False)
            chosen = order_row[batch_index * batch_size:(batch_index + 1) * batch_size]
            offset_row = lax.dynamic_index_in_dim(offset_flat, tile_index, 0, keepdims=False)
            amp_row = lax.dynamic_index_in_dim(amp_flat, tile_index, 0, keepdims=False)
            chosen_offsets = offset_row[chosen]
            chosen_amps = amp_row[chosen]
            top_rows = (tile_row * TILE + chosen_offsets[:, 0] + HALO).astype(jnp.int32)
            left_cols = (tile_col * TILE + chosen_offsets[:, 1] + HALO).astype(jnp.int32)
            patches = jax.vmap(lambda top_index, left_index: lax.dynamic_slice(object_pair, (jnp.int32(0), top_index, left_index), (2, FRAME, FRAME)))(top_rows, left_cols)
            obj_re, obj_im, part_re, part_im = correct(patches[:, 0], patches[:, 1], chosen_amps, probe_re, probe_im, table_re, table_im)
            update_terms = jnp.stack([obj_re, obj_im], axis=1)
            for member in range(batch_size):
                start_at = (jnp.int32(0), top_rows[member], left_cols[member])
                current = lax.dynamic_slice(accum, start_at, (2, FRAME, FRAME))
                accum = lax.dynamic_update_slice(accum, current + update_terms[member], start_at)
            return (accum, probe_acc_re + part_re, probe_acc_im + part_im)
        accum, grad_re, grad_im = lax.fori_loop(0, tile_count, one_tile, (jnp.zeros_like(object_pair), grad_re, grad_im))
        inner = object_pair[:, HALO:-HALO, HALO:-HALO] + OBJECT_RATE * accum[:, HALO:-HALO, HALO:-HALO] / probe_power
        object_pair = jnp.pad(inner, ((0, 0), (HALO, HALO), (HALO, HALO)))
    probe_rate = PROBE_GAIN / (POS_DEV * math.sqrt(N_SY * N_SX))
    final = object_pair[:, HALO:-HALO, HALO:-HALO]
    return (final[0], final[1], probe_re + probe_rate * grad_re, probe_im + probe_rate * grad_im)
```

```python
import functools
import math

import numpy as np

import jax
import jax.numpy as jnp
from jax import lax
from jax.experimental import pallas as pl
from jax.experimental.pallas import tpu as pltpu
from jax.sharding import PartitionSpec as P

MESH = pl.DeviceIdType.MESH
BATCHES = 2
OBJECT_RATE = 0.25
PROBE_GAIN = 4.0
F = 256
H = 128
E = F + 2 * H
ROWS = 16
COLS = 16
VMEM = pl.BlockSpec(memory_space=pltpu.VMEM)
SMEM = pl.BlockSpec(memory_space=pltpu.SMEM)
ANY = pl.BlockSpec(memory_space=pl.ANY)
DIRECTIONS = [(dr, dc) for dr in (-1, 0, 1) for dc in (-1, 0, 1) if (dr, dc) != (0, 0)]
TILE_ROWS = {-1: (H, H), 0: (H, F), 1: (F, H)}
TILE_PLANES = {-1: (1, 1), 0: (1, 2), 1: (2, 1)}
OUTER_ROWS = {-1: (0, H), 0: (H, F), 1: (H + F, H)}
OUTER_PLANES = {-1: (0, 1), 0: (1, 2), 1: (3, 1)}
FRAME_ROWS = {-1: (H + F, H), 0: (H, F), 1: (0, H)}
FRAME_PLANES = {-1: (3, 1), 0: (1, 2), 1: (0, 1)}
INNER_ROWS = {-1: (F, H), 0: (H, F), 1: (H, H)}
INNER_PLANES = {-1: (2, 1), 0: (1, 2), 1: (1, 1)}


def table(frame_size):
    ramp = np.arange(frame_size, dtype=np.int64)
    product = (ramp[:, None] * ramp[None, :]) % frame_size
    angle = np.float32(2.0 * math.pi / frame_size) * product.astype(np.float32)
    scale = np.float32(1.0 / math.sqrt(frame_size))
    return np.cos(angle) * scale, -np.sin(angle) * scale


def dft_operands():
    re, im = table(F)
    left = np.block([[re, -im], [im, re]])
    back_left = np.block([[re, im], [-im, re]])
    right = np.block([[re, im], [-im, re]])
    back_right = np.block([[re, -im], [im, re]])
    return [jnp.asarray(m, jnp.float32).astype(jnp.bfloat16) for m in (left, back_left, right, back_right)]


def part(pair):
    return pl.ds(pair[0], pair[1])


def inside(row, col):
    return (row >= 0) & (row < ROWS) & (col >= 0) & (col < COLS)


def greet_neighbours(row, col):
    barrier = pltpu.get_barrier_semaphore()
    count = jnp.int32(0)
    for dr, dc in DIRECTIONS:
        there = inside(row + dr, col + dc)

        @pl.when(there)
        def _():
            pl.semaphore_signal(barrier, inc=1, device_id=(row + dr, col + dc), device_id_type=MESH)

        count = count + there.astype(jnp.int32)
    pl.semaphore_wait(barrier, count)


def exchange(row, col, make):
    for k, (dr, dc) in enumerate(DIRECTIONS):

        @pl.when(inside(row + dr, col + dc))
        def _():
            for copy in make(k, dr, dc, (row + dr, col + dc)):
                copy.start()


def finish(row, col, make):
    for k, (dr, dc) in enumerate(DIRECTIONS):

        @pl.when(inside(row - dr, col - dc))
        def _():
            for copy in make(k, dr, dc, (row - dr, col - dc)):
                copy.wait_recv()

    for k, (dr, dc) in enumerate(DIRECTIONS):

        @pl.when(inside(row + dr, col + dc))
        def _():
            for copy in make(k, dr, dc, (row + dr, col + dc)):
                copy.wait_send()


def clear_edges(row, col, frame):
    @pl.when(row == 0)
    def _():
        frame[:, :, 0:H, :] = jnp.zeros((2, 4, H, H), jnp.float32)

    @pl.when(row == ROWS - 1)
    def _():
        frame[:, :, H + F : E, :] = jnp.zeros((2, 4, H, H), jnp.float32)

    @pl.when(col == 0)
    def _():
        frame[:, 0] = jnp.zeros((2, E, H), jnp.float32)

    @pl.when(col == COLS - 1)
    def _():
        frame[:, 3] = jnp.zeros((2, E, H), jnp.float32)


def halo_kernel(re_ref, im_ref, frame, send_sem, recv_sem):
    row, col = lax.axis_index("sy"), lax.axis_index("sx")
    greet_neighbours(row, col)

    def make(k, dr, dc, device):
        rows, count = TILE_ROWS[dr]
        plane, planes = TILE_PLANES[dc]
        return [
            pltpu.make_async_remote_copy(
                src_ref=source.at[pl.ds(rows - H, count), pl.ds((plane - 1 + n) * H, H)],
                dst_ref=frame.at[channel, FRAME_PLANES[dc][0] + n, part(FRAME_ROWS[dr])],
                send_sem=send_sem.at[channel, n, k],
                recv_sem=recv_sem.at[channel, n, k],
                device_id=device,
                device_id_type=MESH,
            )
            for channel, source in enumerate((re_ref, im_ref))
            for n in range(planes)
        ]

    exchange(row, col, make)
    clear_edges(row, col, frame)
    for channel, source in enumerate((re_ref, im_ref)):
        for n in range(2):
            frame[channel, 1 + n, H : H + F] = source[:, n * H : (n + 1) * H]
    finish(row, col, make)


def fold_into(row, col, accum, bufs, send_sem, recv_sem, begin, add):
    def make(k, dr, dc, device):
        return [
            pltpu.make_async_remote_copy(
                src_ref=accum.at[:, part(OUTER_PLANES[dc]), part(OUTER_ROWS[dr])],
                dst_ref=bufs[k],
                send_sem=send_sem.at[k],
                recv_sem=recv_sem.at[k],
                device_id=device,
                device_id_type=MESH,
            )
        ]

    exchange(row, col, make)
    begin()
    finish(row, col, make)
    for k, (dr, dc) in enumerate(DIRECTIONS):

        @pl.when(inside(row - dr, col - dc))
        def _():
            add(k, INNER_ROWS[dr], INNER_PLANES[dc])


def mid_kernel(accum, old, frame, b0, b1, b2, b3, b4, b5, b6, b7, send_sem, recv_sem, send2, recv2):
    row, col = lax.axis_index("sy"), lax.axis_index("sx")
    greet_neighbours(row, col)
    bufs = (b0, b1, b2, b3, b4, b5, b6, b7)

    def begin():
        clear_edges(row, col, frame)
        frame[:, 1:3, H : H + F] = old[:, 1:3, H : H + F] + accum[:, 1:3, H : H + F]

    def add(k, rows, planes):
        where = (slice(None), part(planes), part(rows))
        frame[where] = frame[where] + bufs[k][...]

    fold_into(row, col, accum, bufs, send_sem, recv_sem, begin, add)

    def make(k, dr, dc, device):
        return [
            pltpu.make_async_remote_copy(
                src_ref=frame.at[:, part(TILE_PLANES[dc]), part(TILE_ROWS[dr])],
                dst_ref=frame.at[:, part(FRAME_PLANES[dc]), part(FRAME_ROWS[dr])],
                send_sem=send2.at[k],
                recv_sem=recv2.at[k],
                device_id=device,
                device_id_type=MESH,
            )
        ]

    exchange(row, col, make)
    finish(row, col, make)


def fold_kernel(accum, old, out_re, out_im, b0, b1, b2, b3, b4, b5, b6, b7, send_sem, recv_sem):
    row, col = lax.axis_index("sy"), lax.axis_index("sx")
    greet_neighbours(row, col)
    bufs = (b0, b1, b2, b3, b4, b5, b6, b7)
    outs = (out_re, out_im)

    def begin():
        for channel, out in enumerate(outs):
            for n in range(2):
                out[:, n * H : (n + 1) * H] = old[channel, 1 + n, H : H + F] + accum[channel, 1 + n, H : H + F]

    def add(k, rows, planes):
        for channel, out in enumerate(outs):
            for n in range(planes[1]):
                where = (pl.ds(rows[0] - H, rows[1]), pl.ds((planes[0] - 1 + n) * H, H))
                out[where] = out[where] + bufs[k][channel, n]

    fold_into(row, col, accum, bufs, send_sem, recv_sem, begin, add)


def strip_buffers():
    return [
        pltpu.VMEM((2, OUTER_PLANES[dc][1], OUTER_ROWS[dr][1], H), jnp.float32) for dr, dc in DIRECTIONS
    ]


CHUNK1 = 64
CHUNK2 = 16
COLORS = (("x", "y"), ("y", "x"))


def sum_kernel(g, probe, out, r0, w0, r1, w1, r2, w2, r3, w4, s0, q0, s1, q1, s2, q2, s3, q3, s4, q4, s5, q5, s6, q6):
    sy, sx = lax.axis_index("sy"), lax.axis_index("sx")
    here = {
        "y": lax.div(sy, 4),
        "x": lax.div(lax.rem(sx, 8), 2),
        "z": lax.div(sx, 8) * 4 + lax.rem(sy, 4),
        "core": lax.rem(sx, 2),
    }
    size = {"x": 4, "y": 4, "z": 8, "core": 2}
    rate = PROBE_GAIN / (8 * math.sqrt(ROWS * COLS))

    def place(axis, step):
        there = dict(here)
        there[axis] = lax.rem(here[axis] + step, size[axis])
        device = (
            there["y"] * 4 + lax.rem(there["z"], 4),
            lax.div(there["z"], 4) * 8 + there["x"] * 2 + there["core"],
        )
        return there[axis], device

    def send(src, dst, ss, rs, device):
        copy = pltpu.make_async_remote_copy(
            src_ref=src, dst_ref=dst, send_sem=ss, recv_sem=rs, device_id=device, device_id_type=MESH
        )
        copy.start()
        return copy

    barrier = pltpu.get_barrier_semaphore()
    for axis in ("core", "x", "y", "z"):
        for step in range(1, size[axis]):
            pl.semaphore_signal(barrier, inc=1, device_id=place(axis, step)[1], device_id_type=MESH)
    pl.semaphore_wait(barrier, 1 + 3 + 3 + 7)

    core = here["core"]
    other, partner = place("core", 1)
    mine = pl.ds(pl.multiple_of(core * 512, 512), 512)
    theirs = pl.ds(pl.multiple_of(other * 512, 512), 512)
    send(g.at[theirs], r0, s0, q0, partner).wait()
    w0[...] = g[mine] + r0[...]

    copies = []
    for c, (first, second) in enumerate(COLORS):
        for step in (1, 2, 3):
            index, device = place(first, step)
            source = w0.at[pl.ds(pl.multiple_of(c * 256 + index * CHUNK1, CHUNK1), CHUNK1)]
            copies.append(send(source, r1.at[c, step - 1], s1.at[c, step - 1], q1.at[c, step - 1], device))
    for copy in copies:
        copy.wait()
    for c, (first, second) in enumerate(COLORS):
        own = w0[pl.ds(pl.multiple_of(c * 256 + here[first] * CHUNK1, CHUNK1), CHUNK1)]
        w1[c] = (own + r1[c, 0]) + (r1[c, 1] + r1[c, 2])

    copies = []
    for c, (first, second) in enumerate(COLORS):
        for step in (1, 2, 3):
            index, device = place(second, step)
            source = w1.at[c, pl.ds(pl.multiple_of(index * CHUNK2, CHUNK2), CHUNK2)]
            copies.append(send(source, r2.at[c, step - 1], s2.at[c, step - 1], q2.at[c, step - 1], device))
    for copy in copies:
        copy.wait()
    for c, (first, second) in enumerate(COLORS):
        own = w1[c, pl.ds(pl.multiple_of(here[second] * CHUNK2, CHUNK2), CHUNK2)]
        w2[c] = (own + r2[c, 0]) + (r2[c, 1] + r2[c, 2])

    copies = []
    for c in range(2):
        for step in range(1, 8):
            index, device = place("z", step)
            copies.append(send(w2.at[c], r3.at[c, here["z"]], s3.at[c, step - 1], q3.at[c, step - 1], device))
    for c in range(2):
        r3[c, here["z"]] = w2[c]
    for copy in copies:
        copy.wait()
    for c, (first, second) in enumerate(COLORS):
        total = ((r3[c, 0] + r3[c, 1]) + (r3[c, 2] + r3[c, 3])) + ((r3[c, 4] + r3[c, 5]) + (r3[c, 6] + r3[c, 7]))
        start = core * 512 + c * 256 + here[first] * CHUNK1 + here[second] * CHUNK2
        base = probe[pl.ds(pl.multiple_of(start, CHUNK2), CHUNK2)]
        w4[c, pl.ds(pl.multiple_of(here[second] * CHUNK2, CHUNK2), CHUNK2)] = base + rate * total

    copies = []
    for c, (first, second) in enumerate(COLORS):
        spot = w4.at[c, pl.ds(pl.multiple_of(here[second] * CHUNK2, CHUNK2), CHUNK2)]
        for step in (1, 2, 3):
            copies.append(send(spot, spot, s4.at[c, step - 1], q4.at[c, step - 1], place(second, step)[1]))
    for copy in copies:
        copy.wait()

    copies = []
    for c, (first, second) in enumerate(COLORS):
        start = core * 512 + c * 256 + here[first] * CHUNK1
        spot = out.at[pl.ds(pl.multiple_of(start, CHUNK1), CHUNK1)]
        for step in (1, 2, 3):
            copies.append(send(w4.at[c], spot, s5.at[c, step - 1], q5.at[c, step - 1], place(first, step)[1]))
    for c, (first, second) in enumerate(COLORS):
        start = core * 512 + c * 256 + here[first] * CHUNK1
        out[pl.ds(pl.multiple_of(start, CHUNK1), CHUNK1)] = w4[c]
    for copy in copies:
        copy.wait()

    send(out.at[mine], out.at[mine], s6, q6, partner).wait()


def work_kernel(batch, order, offsets, frame, probe_re, probe_im, amps, left, back_left, right, back_right, *rest):
    if batch == 0:
        accum, grad, patch, fields, halves, amp, amp_sem = rest
        grad_in = None
    else:
        grad_in, accum, grad, patch, fields, halves, amp, amp_sem = rest
    size = 4
    loads = []
    for j in range(size):
        p = order[batch * size + j]
        load = pltpu.make_async_copy(amps.at[p], amp.at[j], amp_sem.at[j])
        load.start()
        loads.append(load)

    power = jnp.max(
        probe_re[0] * probe_re[0]
        + probe_im[0] * probe_im[0]
        + (probe_re[1] * probe_re[1] + probe_im[1] * probe_im[1])
    )
    scale = OBJECT_RATE / jnp.full((8, 128), power, jnp.float32)[0:1, 0:1]
    accum[...] = jnp.zeros_like(accum)
    for j in range(size):
        p = order[batch * size + j]
        top = offsets[p, 0] + H
        shift = offsets[p, 1] + H
        for ch in range(2):
            rows = jnp.concatenate([frame[ch, n, pl.ds(top, F), :] for n in range(4)], axis=1)
            patch[j, ch] = pltpu.roll(rows, lax.rem(E - shift, E), 1)[:, :F]
        re, im = patch[j, 0], patch[j, 1]
        for m in range(2):
            at = pl.ds((2 * j + m) * F, F)
            fields[0:F, at] = (probe_re[m] * re - probe_im[m] * im).astype(jnp.bfloat16)
            fields[F : 2 * F, at] = (probe_re[m] * im + probe_im[m] * re).astype(jnp.bfloat16)
    for n in range(2 * size):
        half = jnp.dot(left[...], fields[0 : 2 * F, n * F : (n + 1) * F], preferred_element_type=jnp.float32)
        halves[n * F : (n + 1) * F, 0:F] = half[0:F].astype(jnp.bfloat16)
        halves[n * F : (n + 1) * F, F : 2 * F] = half[F:].astype(jnp.bfloat16)
    for j in range(size):
        far = jnp.dot(halves[2 * j * F : 2 * (j + 1) * F, :], right[...], preferred_element_type=jnp.float32)
        squares = far * far
        intensity = (squares[0:F, 0:F] + squares[0:F, F:]) + (squares[F:, 0:F] + squares[F:, F:])
        loads[j].wait()
        ratio = amp[j] * lax.rsqrt(jnp.maximum(intensity, 1.0))
        for m in range(2):
            at = (2 * j + m) * F
            fields[2 * F : 3 * F, at : at + F] = (far[m * F : (m + 1) * F, 0:F] * ratio).astype(jnp.bfloat16)
            fields[3 * F : 4 * F, at : at + F] = (far[m * F : (m + 1) * F, F:] * ratio).astype(jnp.bfloat16)
    for n in range(2 * size):
        half = jnp.dot(back_left[...], fields[2 * F :, n * F : (n + 1) * F], preferred_element_type=jnp.float32)
        halves[n * F : (n + 1) * F, 0:F] = half[0:F].astype(jnp.bfloat16)
        halves[n * F : (n + 1) * F, F : 2 * F] = half[F:].astype(jnp.bfloat16)
    for j in range(size):
        p = order[batch * size + j]
        top = offsets[p, 0] + H
        shift = offsets[p, 1] + H
        back = jnp.dot(halves[2 * j * F : 2 * (j + 1) * F, :], back_right[...], preferred_element_type=jnp.float32)
        re, im = patch[j, 0], patch[j, 1]
        terms = [None, None]
        for m in range(2):
            at = (2 * j + m) * F
            d_re = back[m * F : (m + 1) * F, 0:F] - fields[0:F, at : at + F].astype(jnp.float32)
            d_im = back[m * F : (m + 1) * F, F:] - fields[F : 2 * F, at : at + F].astype(jnp.float32)
            o_re = probe_re[m] * d_re + probe_im[m] * d_im
            o_im = probe_re[m] * d_im - probe_im[m] * d_re
            g_re = re * d_re + im * d_im
            g_im = re * d_im - im * d_re
            if m == 0:
                terms = [o_re, o_im]
            else:
                terms = [terms[0] + o_re, terms[1] + o_im]
            for ch, g in enumerate((g_re, g_im)):
                if j == 0:
                    grad[ch, m] = g if grad_in is None else grad_in[ch, m] + g
                else:
                    grad[ch, m] = grad[ch, m] + g
        for ch in range(2):
            wide = jnp.concatenate([terms[ch] * scale, jnp.zeros((F, F), jnp.float32)], axis=1)
            wide = pltpu.roll(wide, shift, 1)
            for n in range(4):
                accum[ch, n, pl.ds(top, F), :] += wide[:, n * H : (n + 1) * H]


def local(object_re, object_im, probe_re, probe_im, amplitudes, offsets, visit_order):
    f32 = jnp.float32
    amps = amplitudes.reshape(8, F, F)
    offs = offsets.reshape(8, 2)
    order = visit_order.reshape(8)
    tables = dft_operands()
    frame_shape = jax.ShapeDtypeStruct((2, 4, E, H), f32)
    grad_shape = jax.ShapeDtypeStruct((2, 2, F, F), f32)
    limit = 60 * 1024 * 1024

    def comm(kernel, outs, scratch, ident, n_in):
        return pl.pallas_call(
            kernel,
            out_shape=outs,
            in_specs=[VMEM] * n_in,
            out_specs=[VMEM] * len(outs) if isinstance(outs, list) else VMEM,
            scratch_shapes=scratch,
            compiler_params=pltpu.CompilerParams(
                collective_id=ident, has_side_effects=True, vmem_limit_bytes=limit
            ),
        )

    dma = pltpu.SemaphoreType.DMA

    def work(batch, frame, grad):
        ins = [order, offs, frame, probe_re, probe_im, amps, *tables]
        specs = [SMEM, SMEM, VMEM, VMEM, VMEM, ANY] + [VMEM] * 4
        if grad is not None:
            ins.append(grad)
            specs.append(VMEM)
        return pl.pallas_call(
            functools.partial(work_kernel, batch),
            out_shape=[frame_shape, grad_shape],
            in_specs=specs,
            out_specs=[VMEM, VMEM],
            scratch_shapes=[
                pltpu.VMEM((4, 2, F, F), f32),
                pltpu.VMEM((4 * F, 8 * F), jnp.bfloat16),
                pltpu.VMEM((8 * F, 2 * F), jnp.bfloat16),
                pltpu.VMEM((4, F, F), f32),
                dma((4,)),
            ],
            compiler_params=pltpu.CompilerParams(vmem_limit_bytes=limit),
            cost_estimate=pl.CostEstimate(flops=4_300_000_000, bytes_accessed=10_000_000, transcendentals=262144),
        )(*ins)

    frame = comm(halo_kernel, frame_shape, [dma((2, 2, 8)), dma((2, 2, 8))], 0, 2)(object_re, object_im)
    accum, grad = work(0, frame, None)
    frame = comm(
        mid_kernel, frame_shape, strip_buffers() + [dma((8,))] * 4, 1, 2
    )(accum, frame)
    accum, grad = work(1, frame, grad)
    out = comm(
        fold_kernel, [jax.ShapeDtypeStruct((F, F), f32)] * 2, strip_buffers() + [dma((8,))] * 2, 2, 2
    )(accum, frame)
    probe = jnp.stack([probe_re, probe_im])
    flat = comm(
        sum_kernel,
        jax.ShapeDtypeStruct((1024, F), f32),
        [
            pltpu.VMEM((512, F), f32),
            pltpu.VMEM((512, F), f32),
            pltpu.VMEM((2, 3, CHUNK1, F), f32),
            pltpu.VMEM((2, CHUNK1, F), f32),
            pltpu.VMEM((2, 3, CHUNK2, F), f32),
            pltpu.VMEM((2, CHUNK2, F), f32),
            pltpu.VMEM((2, 8, CHUNK2, F), f32),
            pltpu.VMEM((2, CHUNK1, F), f32),
            dma, dma,
            dma((2, 3)), dma((2, 3)),
            dma((2, 3)), dma((2, 3)),
            dma((2, 7)), dma((2, 7)),
            dma((2, 3)), dma((2, 3)),
            dma((2, 3)), dma((2, 3)),
            dma, dma,
        ],
        3,
        2,
    )(grad.reshape(1024, F), probe.reshape(1024, F))
    new = flat.reshape(2, 2, F, F)
    return (out[0], out[1], new[0], new[1])


def solution(mesh):
    return jax.shard_map(
        local,
        mesh=mesh,
        in_specs=(
            P("sy", "sx"),
            P("sy", "sx"),
            P(),
            P(),
            P("sy", "sx", None, None, None),
            P("sy", "sx", None, None),
            P("sy", "sx", None),
        ),
        out_specs=(P("sy", "sx"), P("sy", "sx"), P(), P()),
        check_vma=False,
    )
```

```python
import functools
import math

import numpy as np

import jax
import jax.numpy as jnp
from jax import lax
from jax.experimental import pallas as pl
from jax.experimental.pallas import tpu as pltpu
from jax.sharding import PartitionSpec as P

MESH = pl.DeviceIdType.MESH
BATCHES = 2
OBJECT_RATE = 0.25
PROBE_GAIN = 4.0
F = 256
H = 128
E = F + 2 * H
ROWS = 16
COLS = 16
SEAM = 8
VMEM = pl.BlockSpec(memory_space=pltpu.VMEM)
SMEM = pl.BlockSpec(memory_space=pltpu.SMEM)
ANY = pl.BlockSpec(memory_space=pl.ANY)
TILE_ROWS = {-1: (H, H), 0: (H, F), 1: (F, H)}
TILE_PLANES = {-1: (1, 1), 0: (1, 2), 1: (2, 1)}
OUTER_ROWS = {-1: (0, H), 0: (H, F), 1: (H + F, H)}
OUTER_PLANES = {-1: (0, 1), 0: (1, 2), 1: (3, 1)}
FRAME_ROWS = {-1: (H + F, H), 0: (H, F), 1: (0, H)}
FRAME_PLANES = {-1: (3, 1), 0: (1, 2), 1: (0, 1)}
INNER_ROWS = {-1: (F, H), 0: (H, F), 1: (H, H)}
INNER_PLANES = {-1: (2, 1), 0: (1, 2), 1: (1, 1)}


def table(frame_size):
    ramp = np.arange(frame_size, dtype=np.int64)
    product = (ramp[:, None] * ramp[None, :]) % frame_size
    angle = np.float32(2.0 * math.pi / frame_size) * product.astype(np.float32)
    scale = np.float32(1.0 / math.sqrt(frame_size))
    return np.cos(angle) * scale, -np.sin(angle) * scale


def dft_operands():
    re, im = table(F)
    left = np.block([[re, -im], [im, re]])
    back_left = np.block([[re, im], [-im, re]])
    right = np.block([[re, im], [-im, re]])
    back_right = np.block([[re, -im], [im, re]])
    return [jnp.asarray(m, jnp.float32).astype(jnp.bfloat16) for m in (left, back_left, right, back_right)]


def part(pair):
    return pl.ds(pair[0], pair[1])


def inside(row, col):
    return (row >= 0) & (row < ROWS) & (col >= 0) & (col < COLS)


def greet(peers):
    barrier = pltpu.get_barrier_semaphore()
    count = jnp.int32(0)
    for there, device in peers:

        @pl.when(there)
        def _():
            pl.semaphore_signal(barrier, inc=1, device_id=device, device_id_type=MESH)

        count = count + there.astype(jnp.int32)
    pl.semaphore_wait(barrier, count)


class Spot:
    def __init__(self):
        self.row, self.col = lax.axis_index("sy"), lax.axis_index("sx")

    def at(self, dr, dc):
        return (self.row + dr, self.col + dc)

    def has(self, dr, dc):
        return inside(self.row + dr, self.col + dc)

    def far(self, dc):
        return self.col == (SEAM - 1 if dc > 0 else SEAM)

    def peers(self):
        near = [(self.has(dr, dc), self.at(dr, dc)) for dr, dc in ((-1, 0), (1, 0), (0, -1), (0, 1))]
        seam = [
            (self.has(dr, dc) & self.far(dc), self.at(dr, dc)) for dr in (-1, 1) for dc in (-1, 1)
        ]
        return near + seam


def remote(src, dst, sems, k, device):
    return pltpu.make_async_remote_copy(
        src_ref=src,
        dst_ref=dst,
        send_sem=sems[0].at[k],
        recv_sem=sems[1].at[k],
        device_id=device,
        device_id_type=MESH,
    )


class Transfers:
    def __init__(self, entries):
        self.entries = entries

    def start(self):
        for sent, received, build in self.entries:

            @pl.when(sent)
            def _():
                build().start()

    def wait_recv(self):
        for sent, received, build in self.entries:

            @pl.when(received)
            def _():
                build().wait_recv()

    def wait_send(self):
        for sent, received, build in self.entries:

            @pl.when(sent)
            def _():
                build().wait_send()


SIDES = (-1, 1)


def clear_edges(row, col, frame):
    @pl.when(row == 0)
    def _():
        frame[:, :, 0:H, :] = jnp.zeros((2, 4, H, H), jnp.float32)

    @pl.when(row == ROWS - 1)
    def _():
        frame[:, :, H + F : E, :] = jnp.zeros((2, 4, H, H), jnp.float32)

    @pl.when(col == 0)
    def _():
        frame[:, 0] = jnp.zeros((2, E, H), jnp.float32)

    @pl.when(col == COLS - 1)
    def _():
        frame[:, 3] = jnp.zeros((2, E, H), jnp.float32)


def halo(spot, frame, upright, level, corner, seam):
    def strip(dr, planes, rows_from, to_rows, to_planes, sems, k, device):
        return lambda: remote(
            frame.at[:, part(planes), part(rows_from)], frame.at[:, part(to_planes), part(to_rows)], sems, k, device
        )

    vertical = Transfers(
        [
            (
                spot.has(dr, 0),
                spot.has(-dr, 0),
                strip(dr, (1, 2), TILE_ROWS[dr], FRAME_ROWS[dr], (1, 2), upright, k, spot.at(dr, 0)),
            )
            for k, dr in enumerate(SIDES)
        ]
    )
    across = Transfers(
        [
            (
                spot.has(dr, dc) & spot.far(dc),
                spot.has(-dr, -dc) & spot.far(-dc),
                strip(dr, TILE_PLANES[dc], TILE_ROWS[dr], FRAME_ROWS[dr], FRAME_PLANES[dc], seam, 2 * k + n, spot.at(dr, dc)),
            )
            for k, dr in enumerate(SIDES)
            for n, dc in enumerate(SIDES)
        ]
    )
    middle = Transfers(
        [
            (
                spot.has(0, dc),
                spot.has(0, -dc),
                strip(0, TILE_PLANES[dc], (H, F), (H, F), FRAME_PLANES[dc], level, n, spot.at(0, dc)),
            )
            for n, dc in enumerate(SIDES)
        ]
    )
    corners = Transfers(
        [
            (
                spot.has(side, 0) & spot.has(0, dc) & ~spot.far(dc),
                spot.has(side, 0) & spot.has(0, -dc) & ~spot.far(-dc),
                strip(0, TILE_PLANES[dc], OUTER_ROWS[side], OUTER_ROWS[side], FRAME_PLANES[dc], corner, 2 * k + n, spot.at(0, dc)),
            )
            for k, side in enumerate(SIDES)
            for n, dc in enumerate(SIDES)
        ]
    )
    vertical.start()
    across.start()
    middle.start()
    clear_edges(spot.row, spot.col, frame)
    vertical.wait_recv()
    corners.start()
    for transfers in (middle, across, corners):
        transfers.wait_recv()
    for transfers in (vertical, middle, across, corners):
        transfers.wait_send()


def halo_kernel(re_ref, im_ref, frame, *sems):
    spot = Spot()
    for channel, source in enumerate((re_ref, im_ref)):
        for n in range(2):
            frame[channel, 1 + n, H : H + F] = source[:, n * H : (n + 1) * H]
    greet(spot.peers())
    halo(spot, frame, *pairs(sems))


def pairs(sems):
    return [(sems[i], sems[i + 1]) for i in range(0, len(sems), 2)]


def fold_parts(spot, accum, cbuf, mbuf, vbuf, fbuf, stack, upright, level, corner, seam):
    def strip(planes, rows, buf, sems, k, device):
        return lambda: remote(accum.at[:, part(planes), part(rows)], buf, sems, k, device)

    corners = Transfers(
        [
            (
                spot.has(side, 0) & spot.has(0, dc) & ~spot.far(dc),
                spot.has(side, 0) & spot.has(0, -dc) & ~spot.far(-dc),
                strip(OUTER_PLANES[dc], OUTER_ROWS[side], cbuf.at[2 * k + n], corner, 2 * k + n, spot.at(0, dc)),
            )
            for k, side in enumerate(SIDES)
            for n, dc in enumerate(SIDES)
        ]
    )
    across = Transfers(
        [
            (
                spot.has(dr, dc) & spot.far(dc),
                spot.has(-dr, -dc) & spot.far(-dc),
                strip(OUTER_PLANES[dc], OUTER_ROWS[dr], fbuf.at[2 * k + n], seam, 2 * k + n, spot.at(dr, dc)),
            )
            for k, dr in enumerate(SIDES)
            for n, dc in enumerate(SIDES)
        ]
    )
    middle = Transfers(
        [
            (
                spot.has(0, dc),
                spot.has(0, -dc),
                strip(OUTER_PLANES[dc], (H, F), mbuf.at[n], level, n, spot.at(0, dc)),
            )
            for n, dc in enumerate(SIDES)
        ]
    )
    vertical = Transfers(
        [
            (
                spot.has(dr, 0),
                spot.has(-dr, 0),
                lambda k=k, dr=dr: remote(stack.at[k], vbuf.at[k], upright, k, spot.at(dr, 0)),
            )
            for k, dr in enumerate(SIDES)
        ]
    )

    def begin():
        corners.start()
        across.start()
        middle.start()

    def turn():
        for k, side in enumerate(SIDES):
            stack[k] = accum[:, 1:3, part(OUTER_ROWS[side])]
        corners.wait_recv()
        for (_, received, _), (k, n) in zip(corners.entries, [(k, n) for k in range(2) for n in range(2)]):

            @pl.when(received)
            def _():
                plane = INNER_PLANES[SIDES[n]][0] - 1
                stack[k, :, plane] = stack[k, :, plane] + cbuf[2 * k + n][:, 0]

        vertical.start()

    def end(add):
        middle.wait_recv()
        for n, dc in enumerate(SIDES):

            @pl.when(spot.has(0, -dc))
            def _():
                add(mbuf.at[n], (H, F), INNER_PLANES[dc])

        vertical.wait_recv()
        for k, dr in enumerate(SIDES):

            @pl.when(spot.has(-dr, 0))
            def _():
                add(vbuf.at[k], INNER_ROWS[dr], (1, 2))

        across.wait_recv()
        for (_, received, _), (k, n) in zip(across.entries, [(k, n) for k in range(2) for n in range(2)]):

            @pl.when(received)
            def _():
                add(fbuf.at[2 * k + n], INNER_ROWS[SIDES[k]], INNER_PLANES[SIDES[n]])

        for transfers in (corners, across, middle, vertical):
            transfers.wait_send()

    return begin, turn, end


def mid_kernel(accum, old, frame, cbuf, mbuf, vbuf, fbuf, stack, *sems):
    spot = Spot()
    greet(spot.peers())
    sems = pairs(sems)
    begin, turn, end = fold_parts(spot, accum, cbuf, mbuf, vbuf, fbuf, stack, *sems[:4])
    begin()
    frame[:, 1:3, H : H + F] = old[:, 1:3, H : H + F] + accum[:, 1:3, H : H + F]
    turn()

    def add(buf, rows, planes):
        where = (slice(None), part(planes), part(rows))
        frame[where] = frame[where] + buf[...]

    end(add)
    halo(spot, frame, *sems[4:])


def fold_buffers():
    f32 = jnp.float32
    return [
        pltpu.VMEM((4, 2, 1, H, H), f32),
        pltpu.VMEM((2, 2, 1, F, H), f32),
        pltpu.VMEM((2, 2, 2, H, H), f32),
        pltpu.VMEM((4, 2, 1, H, H), f32),
        pltpu.VMEM((2, 2, 2, H, H), f32),
    ]


def exchange_sems():
    dma = pltpu.SemaphoreType.DMA
    return [dma((2,)), dma((2,)), dma((2,)), dma((2,)), dma((4,)), dma((4,)), dma((4,)), dma((4,))]


CHUNK1 = 64
CHUNK2 = 16
COLORS = (("x", "y"), ("y", "x"))


def last_kernel(accum, old, g, probe, out_re, out_im, out, cbuf, mbuf, vbuf, fbuf, stack, *rest):
    exchange, rest = rest[:8], rest[8:]
    r0, w0, r1, w1, r2, w2, r3, w4, s0, q0, s1, q1, s2, q2, s3, q3, s4, q4, s5, q5, s6, q6 = rest
    spot = Spot()
    sy, sx = lax.axis_index("sy"), lax.axis_index("sx")
    here = {
        "y": lax.div(sy, 4),
        "x": lax.div(lax.rem(sx, 8), 2),
        "z": lax.div(sx, 8) * 4 + lax.rem(sy, 4),
        "core": lax.rem(sx, 2),
    }
    size = {"x": 4, "y": 4, "z": 8, "core": 2}
    rate = PROBE_GAIN / (8 * math.sqrt(ROWS * COLS))

    def place(axis, step):
        there = dict(here)
        there[axis] = lax.rem(here[axis] + step, size[axis])
        device = (
            there["y"] * 4 + lax.rem(there["z"], 4),
            lax.div(there["z"], 4) * 8 + there["x"] * 2 + there["core"],
        )
        return there[axis], device

    def send(src, dst, ss, rs, device):
        copy = pltpu.make_async_remote_copy(
            src_ref=src, dst_ref=dst, send_sem=ss, recv_sem=rs, device_id=device, device_id_type=MESH
        )
        copy.start()
        return copy

    begin, turn, end = fold_parts(spot, accum, cbuf, mbuf, vbuf, fbuf, stack, *pairs(exchange))
    yes = sy >= 0
    greet(
        spot.peers()
        + [(yes, place(axis, step)[1]) for axis in ("core", "x", "y", "z") for step in range(1, size[axis])]
    )

    core = here["core"]
    other, partner = place("core", 1)
    mine = pl.ds(pl.multiple_of(core * 512, 512), 512)
    theirs = pl.ds(pl.multiple_of(other * 512, 512), 512)
    first_copy = send(g.at[theirs], r0, s0, q0, partner)
    begin()
    first_copy.wait()
    w0[...] = g[mine] + r0[...]

    copies = []
    for c, (first, second) in enumerate(COLORS):
        for step in (1, 2, 3):
            index, device = place(first, step)
            source = w0.at[pl.ds(pl.multiple_of(c * 256 + index * CHUNK1, CHUNK1), CHUNK1)]
            copies.append(send(source, r1.at[c, step - 1], s1.at[c, step - 1], q1.at[c, step - 1], device))
    turn()
    for copy in copies:
        copy.wait()
    for c, (first, second) in enumerate(COLORS):
        own = w0[pl.ds(pl.multiple_of(c * 256 + here[first] * CHUNK1, CHUNK1), CHUNK1)]
        w1[c] = (own + r1[c, 0]) + (r1[c, 1] + r1[c, 2])

    copies = []
    for c, (first, second) in enumerate(COLORS):
        for step in (1, 2, 3):
            index, device = place(second, step)
            source = w1.at[c, pl.ds(pl.multiple_of(index * CHUNK2, CHUNK2), CHUNK2)]
            copies.append(send(source, r2.at[c, step - 1], s2.at[c, step - 1], q2.at[c, step - 1], device))
    for copy in copies:
        copy.wait()
    for c, (first, second) in enumerate(COLORS):
        own = w1[c, pl.ds(pl.multiple_of(here[second] * CHUNK2, CHUNK2), CHUNK2)]
        w2[c] = (own + r2[c, 0]) + (r2[c, 1] + r2[c, 2])

    copies = []
    for c in range(2):
        for step in range(1, 8):
            index, device = place("z", step)
            copies.append(send(w2.at[c], r3.at[c, here["z"]], s3.at[c, step - 1], q3.at[c, step - 1], device))
    for c in range(2):
        r3[c, here["z"]] = w2[c]
    outs = (out_re, out_im)
    for channel, tile in enumerate(outs):
        for n in range(2):
            tile[:, n * H : (n + 1) * H] = old[channel, 1 + n, H : H + F] + accum[channel, 1 + n, H : H + F]

    def add(buf, rows, planes):
        for channel, tile in enumerate(outs):
            for n in range(planes[1]):
                where = (pl.ds(rows[0] - H, rows[1]), pl.ds((planes[0] - 1 + n) * H, H))
                tile[where] = tile[where] + buf[channel, n]

    end(add)
    for copy in copies:
        copy.wait()
    for c, (first, second) in enumerate(COLORS):
        total = ((r3[c, 0] + r3[c, 1]) + (r3[c, 2] + r3[c, 3])) + ((r3[c, 4] + r3[c, 5]) + (r3[c, 6] + r3[c, 7]))
        start = core * 512 + c * 256 + here[first] * CHUNK1 + here[second] * CHUNK2
        base = probe[pl.ds(pl.multiple_of(start, CHUNK2), CHUNK2)]
        w4[c, pl.ds(pl.multiple_of(here[second] * CHUNK2, CHUNK2), CHUNK2)] = base + rate * total

    copies = []
    for c, (first, second) in enumerate(COLORS):
        spot = w4.at[c, pl.ds(pl.multiple_of(here[second] * CHUNK2, CHUNK2), CHUNK2)]
        for step in (1, 2, 3):
            copies.append(send(spot, spot, s4.at[c, step - 1], q4.at[c, step - 1], place(second, step)[1]))
    for copy in copies:
        copy.wait()

    copies = []
    for c, (first, second) in enumerate(COLORS):
        start = core * 512 + c * 256 + here[first] * CHUNK1
        spot = out.at[pl.ds(pl.multiple_of(start, CHUNK1), CHUNK1)]
        for step in (1, 2, 3):
            copies.append(send(w4.at[c], spot, s5.at[c, step - 1], q5.at[c, step - 1], place(first, step)[1]))
    for c, (first, second) in enumerate(COLORS):
        start = core * 512 + c * 256 + here[first] * CHUNK1
        out[pl.ds(pl.multiple_of(start, CHUNK1), CHUNK1)] = w4[c]
    for copy in copies:
        copy.wait()

    send(out.at[mine], out.at[mine], s6, q6, partner).wait()


def work_kernel(batch, order, offsets, frame, probe_re, probe_im, amps, left, back_left, right, back_right, *rest):
    if batch == 0:
        accum, grad, patch, fields, halves, amp, amp_sem = rest
        grad_in = None
    else:
        grad_in, accum, grad, patch, fields, halves, amp, amp_sem = rest
    size = 4
    loads = []
    for j in range(size):
        p = order[batch * size + j]
        load = pltpu.make_async_copy(amps.at[p], amp.at[j], amp_sem.at[j])
        load.start()
        loads.append(load)

    power = jnp.max(
        probe_re[0] * probe_re[0]
        + probe_im[0] * probe_im[0]
        + (probe_re[1] * probe_re[1] + probe_im[1] * probe_im[1])
    )
    scale = OBJECT_RATE / jnp.full((8, 128), power, jnp.float32)[0:1, 0:1]
    accum[...] = jnp.zeros_like(accum)
    for j in range(size):
        p = order[batch * size + j]
        top = offsets[p, 0] + H
        shift = offsets[p, 1] + H
        for ch in range(2):
            rows = jnp.concatenate([frame[ch, n, pl.ds(top, F), :] for n in range(4)], axis=1)
            patch[j, ch] = pltpu.roll(rows, lax.rem(E - shift, E), 1)[:, :F]
        re, im = patch[j, 0], patch[j, 1]
        for m in range(2):
            at = pl.ds((2 * j + m) * F, F)
            fields[0:F, at] = (probe_re[m] * re - probe_im[m] * im).astype(jnp.bfloat16)
            fields[F : 2 * F, at] = (probe_re[m] * im + probe_im[m] * re).astype(jnp.bfloat16)
    for n in range(2 * size):
        half = jnp.dot(left[...], fields[0 : 2 * F, n * F : (n + 1) * F], preferred_element_type=jnp.float32)
        halves[n * F : (n + 1) * F, 0:F] = half[0:F].astype(jnp.bfloat16)
        halves[n * F : (n + 1) * F, F : 2 * F] = half[F:].astype(jnp.bfloat16)
    for j in range(size):
        far = jnp.dot(halves[2 * j * F : 2 * (j + 1) * F, :], right[...], preferred_element_type=jnp.float32)
        squares = far * far
        intensity = (squares[0:F, 0:F] + squares[0:F, F:]) + (squares[F:, 0:F] + squares[F:, F:])
        loads[j].wait()
        ratio = amp[j] * lax.rsqrt(jnp.maximum(intensity, 1.0))
        for m in range(2):
            at = (2 * j + m) * F
            fields[2 * F : 3 * F, at : at + F] = (far[m * F : (m + 1) * F, 0:F] * ratio).astype(jnp.bfloat16)
            fields[3 * F : 4 * F, at : at + F] = (far[m * F : (m + 1) * F, F:] * ratio).astype(jnp.bfloat16)
    for n in range(2 * size):
        half = jnp.dot(back_left[...], fields[2 * F :, n * F : (n + 1) * F], preferred_element_type=jnp.float32)
        halves[n * F : (n + 1) * F, 0:F] = half[0:F].astype(jnp.bfloat16)
        halves[n * F : (n + 1) * F, F : 2 * F] = half[F:].astype(jnp.bfloat16)
    for j in range(size):
        p = order[batch * size + j]
        top = offsets[p, 0] + H
        shift = offsets[p, 1] + H
        back = jnp.dot(halves[2 * j * F : 2 * (j + 1) * F, :], back_right[...], preferred_element_type=jnp.float32)
        re, im = patch[j, 0], patch[j, 1]
        terms = [None, None]
        for m in range(2):
            at = (2 * j + m) * F
            d_re = back[m * F : (m + 1) * F, 0:F] - fields[0:F, at : at + F].astype(jnp.float32)
            d_im = back[m * F : (m + 1) * F, F:] - fields[F : 2 * F, at : at + F].astype(jnp.float32)
            o_re = probe_re[m] * d_re + probe_im[m] * d_im
            o_im = probe_re[m] * d_im - probe_im[m] * d_re
            g_re = re * d_re + im * d_im
            g_im = re * d_im - im * d_re
            if m == 0:
                terms = [o_re, o_im]
            else:
                terms = [terms[0] + o_re, terms[1] + o_im]
            for ch, g in enumerate((g_re, g_im)):
                if j == 0:
                    grad[ch, m] = g if grad_in is None else grad_in[ch, m] + g
                else:
                    grad[ch, m] = grad[ch, m] + g
        for ch in range(2):
            wide = jnp.concatenate([terms[ch] * scale, jnp.zeros((F, F), jnp.float32)], axis=1)
            wide = pltpu.roll(wide, shift, 1)
            for n in range(4):
                accum[ch, n, pl.ds(top, F), :] += wide[:, n * H : (n + 1) * H]


def local(object_re, object_im, probe_re, probe_im, amplitudes, offsets, visit_order):
    f32 = jnp.float32
    amps = amplitudes.reshape(8, F, F)
    offs = offsets.reshape(8, 2)
    order = visit_order.reshape(8)
    tables = dft_operands()
    frame_shape = jax.ShapeDtypeStruct((2, 4, E, H), f32)
    grad_shape = jax.ShapeDtypeStruct((2, 2, F, F), f32)
    limit = 60 * 1024 * 1024

    def comm(kernel, outs, scratch, ident, n_in):
        return pl.pallas_call(
            kernel,
            out_shape=outs,
            in_specs=[VMEM] * n_in,
            out_specs=[VMEM] * len(outs) if isinstance(outs, list) else VMEM,
            scratch_shapes=scratch,
            compiler_params=pltpu.CompilerParams(
                collective_id=ident, has_side_effects=True, vmem_limit_bytes=limit
            ),
        )

    dma = pltpu.SemaphoreType.DMA

    def work(batch, frame, grad):
        ins = [order, offs, frame, probe_re, probe_im, amps, *tables]
        specs = [SMEM, SMEM, VMEM, VMEM, VMEM, ANY] + [VMEM] * 4
        if grad is not None:
            ins.append(grad)
            specs.append(VMEM)
        return pl.pallas_call(
            functools.partial(work_kernel, batch),
            out_shape=[frame_shape, grad_shape],
            in_specs=specs,
            out_specs=[VMEM, VMEM],
            scratch_shapes=[
                pltpu.VMEM((4, 2, F, F), f32),
                pltpu.VMEM((4 * F, 8 * F), jnp.bfloat16),
                pltpu.VMEM((8 * F, 2 * F), jnp.bfloat16),
                pltpu.VMEM((4, F, F), f32),
                dma((4,)),
            ],
            compiler_params=pltpu.CompilerParams(vmem_limit_bytes=limit),
            cost_estimate=pl.CostEstimate(flops=4_300_000_000, bytes_accessed=10_000_000, transcendentals=262144),
        )(*ins)

    frame = comm(halo_kernel, frame_shape, exchange_sems(), 0, 2)(object_re, object_im)
    accum, grad = work(0, frame, None)
    frame = comm(mid_kernel, frame_shape, fold_buffers() + exchange_sems() + exchange_sems(), 1, 2)(accum, frame)
    accum, grad = work(1, frame, grad)
    probe = jnp.stack([probe_re, probe_im])
    tile_shape = jax.ShapeDtypeStruct((F, F), f32)
    out_re, out_im, flat = comm(
        last_kernel,
        [tile_shape, tile_shape, jax.ShapeDtypeStruct((1024, F), f32)],
        fold_buffers()
        + exchange_sems()
        + [
            pltpu.VMEM((512, F), f32),
            pltpu.VMEM((512, F), f32),
            pltpu.VMEM((2, 3, CHUNK1, F), f32),
            pltpu.VMEM((2, CHUNK1, F), f32),
            pltpu.VMEM((2, 3, CHUNK2, F), f32),
            pltpu.VMEM((2, CHUNK2, F), f32),
            pltpu.VMEM((2, 8, CHUNK2, F), f32),
            pltpu.VMEM((2, CHUNK1, F), f32),
            dma, dma,
            dma((2, 3)), dma((2, 3)),
            dma((2, 3)), dma((2, 3)),
            dma((2, 7)), dma((2, 7)),
            dma((2, 3)), dma((2, 3)),
            dma((2, 3)), dma((2, 3)),
            dma, dma,
        ],
        2,
        4,
    )(accum, frame, grad.reshape(1024, F), probe.reshape(1024, F))
    new = flat.reshape(2, 2, F, F)
    return (out_re, out_im, new[0], new[1])


def solution(mesh):
    return jax.shard_map(
        local,
        mesh=mesh,
        in_specs=(
            P("sy", "sx"),
            P("sy", "sx"),
            P(),
            P(),
            P("sy", "sx", None, None, None),
            P("sy", "sx", None, None),
            P("sy", "sx", None),
        ),
        out_specs=(P("sy", "sx"), P("sy", "sx"), P(), P()),
        check_vma=False,
    )
```

```python
import functools
import math

import numpy as np

import jax
import jax.numpy as jnp
from jax import lax
from jax.experimental import pallas as pl
from jax.experimental.pallas import tpu as pltpu
from jax.sharding import PartitionSpec as P

MESH = pl.DeviceIdType.MESH
BATCHES = 2
OBJECT_RATE = 0.25
PROBE_GAIN = 4.0
F = 256
H = 128
E = F + 2 * H
ROWS = 16
COLS = 16
SEAM = 8
VMEM = pl.BlockSpec(memory_space=pltpu.VMEM)
SMEM = pl.BlockSpec(memory_space=pltpu.SMEM)
ANY = pl.BlockSpec(memory_space=pl.ANY)
TILE_ROWS = {-1: (H, H), 0: (H, F), 1: (F, H)}
TILE_PLANES = {-1: (1, 1), 0: (1, 2), 1: (2, 1)}
OUTER_ROWS = {-1: (0, H), 0: (H, F), 1: (H + F, H)}
OUTER_PLANES = {-1: (0, 1), 0: (1, 2), 1: (3, 1)}
FRAME_ROWS = {-1: (H + F, H), 0: (H, F), 1: (0, H)}
FRAME_PLANES = {-1: (3, 1), 0: (1, 2), 1: (0, 1)}
INNER_ROWS = {-1: (F, H), 0: (H, F), 1: (H, H)}
INNER_PLANES = {-1: (2, 1), 0: (1, 2), 1: (1, 1)}


def table(frame_size):
    ramp = np.arange(frame_size, dtype=np.int64)
    product = (ramp[:, None] * ramp[None, :]) % frame_size
    angle = np.float32(2.0 * math.pi / frame_size) * product.astype(np.float32)
    scale = np.float32(1.0 / math.sqrt(frame_size))
    return np.cos(angle) * scale, -np.sin(angle) * scale


def dft_operands():
    re, im = table(F)
    left = np.block([[re, -im], [im, re]])
    back_left = np.block([[re, im], [-im, re]])
    right = np.block([[re, im], [-im, re]])
    back_right = np.block([[re, -im], [im, re]])
    return [jnp.asarray(m, jnp.float32).astype(jnp.bfloat16) for m in (left, back_left, right, back_right)]


def part(pair):
    return pl.ds(pair[0], pair[1])


def inside(row, col):
    return (row >= 0) & (row < ROWS) & (col >= 0) & (col < COLS)


def greet(peers):
    barrier = pltpu.get_barrier_semaphore()
    count = jnp.int32(0)
    for there, device in peers:

        @pl.when(there)
        def _():
            pl.semaphore_signal(barrier, inc=1, device_id=device, device_id_type=MESH)

        count = count + there.astype(jnp.int32)
    pl.semaphore_wait(barrier, count)


class Spot:
    def __init__(self):
        self.row, self.col = lax.axis_index("sy"), lax.axis_index("sx")
        self.half = lax.div(self.col, SEAM)
        self.seat = lax.rem(self.col, SEAM)
        self.seam = (self.col == SEAM - 1) | (self.col == SEAM)
        self.edge = (self.row, SEAM - 1 + self.half)
        self.beyond = (self.row, SEAM - self.half)

    def at(self, dr, dc):
        return (self.row + dr, self.col + dc)

    def has(self, dr, dc):
        return inside(self.row + dr, self.col + dc)

    def far(self, dc):
        return self.col == (SEAM - 1 if dc > 0 else SEAM)

    def peers(self):
        near = [(self.has(dr, dc), self.at(dr, dc)) for dr, dc in ((-1, 0), (1, 0), (0, -1), (0, 1))]
        diagonal = [
            (self.has(dr, dc) & self.far(dc), self.at(dr, dc)) for dr in (-1, 1) for dc in (-1, 1)
        ]
        row, col = self.row, self.col
        relays = [
            (self.seam & (col != c) & (jnp.abs(col - c) != 1), (row, jnp.int32(c))) for c in range(COLS)
        ]
        edges = [(~self.seam & (jnp.abs(col - c) != 1), (row, jnp.int32(c))) for c in (SEAM - 1, SEAM)]
        return near + diagonal + relays[: SEAM - 1] + relays[SEAM + 1 :] + [
            (self.seam & (there), device) for there, device in relays[SEAM - 1 : SEAM + 1]
        ] + edges


def remote(src, dst, sems, at, device):
    return pltpu.make_async_remote_copy(
        src_ref=src,
        dst_ref=dst,
        send_sem=sems[0].at[at],
        recv_sem=sems[1].at[at],
        device_id=device,
        device_id_type=MESH,
    )


class Transfers:
    def __init__(self, entries):
        self.entries = entries

    def start(self):
        for sent, received, build in self.entries:

            @pl.when(sent)
            def _():
                build().start()

    def wait_recv(self):
        for sent, received, build in self.entries:

            @pl.when(received)
            def _():
                build().wait_recv()

    def wait_send(self):
        for sent, received, build in self.entries:

            @pl.when(sent)
            def _():
                build().wait_send()


SIDES = (-1, 1)


def clear_edges(row, col, frame):
    @pl.when(row == 0)
    def _():
        frame[:, :, 0:H, :] = jnp.zeros((2, 4, H, H), jnp.float32)

    @pl.when(row == ROWS - 1)
    def _():
        frame[:, :, H + F : E, :] = jnp.zeros((2, 4, H, H), jnp.float32)

    @pl.when(col == 0)
    def _():
        frame[:, 0] = jnp.zeros((2, E, H), jnp.float32)

    @pl.when(col == COLS - 1)
    def _():
        frame[:, 3] = jnp.zeros((2, E, H), jnp.float32)


FOUR = [(k, n) for k in range(2) for n in range(2)]
SLICE = F // SEAM


class Relay:
    def __init__(self, spot, source, target, held, first, second):
        self.spot, self.source, self.target, self.held = spot, source, target, held
        self.first, self.second = first, second

    def out(self, q):
        spot = self.spot
        device = (spot.row, spot.half * SEAM + q)
        return remote(self.source(q * SLICE), self.held, self.first, q, device)

    def arrive(self):
        return pltpu.make_async_remote_copy(
            src_ref=self.held, dst_ref=self.held, send_sem=self.first[0].at[0],
            recv_sem=self.first[1].at[self.spot.seat], device_id=self.spot.edge, device_id_type=MESH,
        )

    def on(self, q, src):
        return remote(src, self.target(pl.multiple_of(q * SLICE, SLICE)), self.second, q, self.spot.beyond)

    def start(self):
        spot = self.spot
        for q in range(SEAM):

            @pl.when(spot.seam & (spot.seat != q))
            def _():
                self.out(q).start()

        for half, q in ((0, SEAM - 1), (1, 0)):

            @pl.when(spot.seam & (spot.half == half))
            def _():
                self.on(q, self.source(q * SLICE)).start()

    def turn(self):
        @pl.when(~self.spot.seam)
        def _():
            self.arrive().wait_recv()
            self.on(self.spot.seat, self.held).start()

    def wait_recv(self):
        @pl.when(self.spot.seam)
        def _():
            for q in range(SEAM):
                self.on(q, self.held).wait_recv()

    def wait_send(self):
        spot = self.spot

        @pl.when(~spot.seam)
        def _():
            self.on(spot.seat, self.held).wait_send()

        for q in range(SEAM):

            @pl.when(spot.seam & (spot.seat != q))
            def _():
                self.out(q).wait_send()

        for half, q in ((0, SEAM - 1), (1, 0)):

            @pl.when(spot.seam & (spot.half == half))
            def _():
                self.on(q, self.held).wait_send()


class Halo:
    def __init__(self, spot, frame, held, upright, level, corner, seam, first, second):
        self.spot, self.frame = spot, frame

        def strip(ch, dr, planes, rows_from, to_rows, to_planes, sems, k, device):
            c = pl.ds(ch, 1)
            return lambda: remote(
                frame.at[c, part(planes), part(rows_from)], frame.at[c, part(to_planes), part(to_rows)], sems, (ch, k), device
            )

        def both(make):
            return [Transfers(make(ch)) for ch in range(2)]

        self.vertical = both(lambda ch: [
            (
                spot.has(dr, 0),
                spot.has(-dr, 0),
                strip(ch, dr, (1, 2), TILE_ROWS[dr], FRAME_ROWS[dr], (1, 2), upright, k, spot.at(dr, 0)),
            )
            for k, dr in enumerate(SIDES)
        ])
        self.across = both(lambda ch: [
            (
                spot.has(dr, dc) & spot.far(dc),
                spot.has(-dr, -dc) & spot.far(-dc),
                strip(ch, dr, TILE_PLANES[dc], TILE_ROWS[dr], FRAME_ROWS[dr], FRAME_PLANES[dc], seam, 2 * k + n, spot.at(dr, dc)),
            )
            for k, dr in enumerate(SIDES)
            for n, dc in enumerate(SIDES)
        ])
        self.middle = both(lambda ch: [
            (
                spot.has(0, dc) & ~spot.far(dc),
                spot.has(0, -dc) & ~spot.far(-dc),
                strip(ch, 0, TILE_PLANES[dc], (H, F), (H, F), FRAME_PLANES[dc], level, n, spot.at(0, dc)),
            )
            for n, dc in enumerate(SIDES)
        ])
        self.corners = both(lambda ch: [
            (
                spot.has(side, 0) & spot.has(0, dc) & ~spot.far(dc),
                spot.has(side, 0) & spot.has(0, -dc) & ~spot.far(-dc),
                strip(ch, 0, TILE_PLANES[dc], OUTER_ROWS[side], OUTER_ROWS[side], FRAME_PLANES[dc], corner, 2 * k + n, spot.at(0, dc)),
            )
            for k, side in enumerate(SIDES)
            for n, dc in enumerate(SIDES)
        ])
        half = spot.half
        self.relay = Relay(
            spot,
            lambda row: frame.at[:, pl.ds(2 - half, 1), pl.ds(H + row, SLICE)],
            lambda row: frame.at[:, pl.ds(3 * half, 1), pl.ds(H + row, SLICE)],
            held, first, second,
        )

    def begin(self, ch):
        self.vertical[ch].start()
        self.across[ch].start()

    def aside(self):
        self.relay.start()
        self.middle[0].start()
        self.middle[1].start()
        self.relay.turn()

    def end(self):
        for ch in range(2):
            self.vertical[ch].wait_recv()
            self.corners[ch].start()
        for ch in range(2):
            self.middle[ch].wait_recv()
        self.relay.wait_recv()
        for ch in range(2):
            for transfers in (self.across[ch], self.corners[ch]):
                transfers.wait_recv()
        for ch in range(2):
            for transfers in (self.vertical[ch], self.middle[ch], self.across[ch], self.corners[ch]):
                transfers.wait_send()
        self.relay.wait_send()


def halo_kernel(re_ref, im_ref, frame, held, *sems):
    spot = Spot()
    for channel, source in enumerate((re_ref, im_ref)):
        for n in range(2):
            frame[channel, 1 + n, H : H + F] = source[:, n * H : (n + 1) * H]
    greet(spot.peers())
    halo = Halo(spot, frame, held, *pairs(sems))
    halo.begin(0)
    halo.begin(1)
    halo.aside()
    clear_edges(spot.row, spot.col, frame)
    halo.end()


def pairs(sems):
    return [(sems[i], sems[i + 1]) for i in range(0, len(sems), 2)]


class Fold:
    def __init__(self, spot, accum, cbuf, mbuf, vbuf, fbuf, stack, held, upright, level, corner, seam, first, second):
        self.spot, self.accum, self.stack = spot, accum, stack
        self.cbuf, self.mbuf, self.vbuf, self.fbuf = cbuf, mbuf, vbuf, fbuf

        def strip(ch, planes, rows, buf, sems, k, device):
            return lambda: remote(accum.at[ch, part(planes), part(rows)], buf.at[ch, k], sems, (ch, k), device)

        def both(make):
            return [Transfers(make(ch)) for ch in range(2)]

        self.corners = both(lambda ch: [
            (
                spot.has(side, 0) & spot.has(0, dc) & ~spot.far(dc),
                spot.has(side, 0) & spot.has(0, -dc) & ~spot.far(-dc),
                strip(ch, OUTER_PLANES[dc], OUTER_ROWS[side], cbuf, corner, 2 * k + n, spot.at(0, dc)),
            )
            for k, side in enumerate(SIDES)
            for n, dc in enumerate(SIDES)
        ])
        self.across = both(lambda ch: [
            (
                spot.has(dr, dc) & spot.far(dc),
                spot.has(-dr, -dc) & spot.far(-dc),
                strip(ch, OUTER_PLANES[dc], OUTER_ROWS[dr], fbuf, seam, 2 * k + n, spot.at(dr, dc)),
            )
            for k, dr in enumerate(SIDES)
            for n, dc in enumerate(SIDES)
        ])
        self.middle = both(lambda ch: [
            (
                spot.has(0, dc) & ~spot.far(dc),
                spot.has(0, -dc) & ~spot.far(-dc),
                strip(ch, OUTER_PLANES[dc], (H, F), mbuf, level, n, spot.at(0, dc)),
            )
            for n, dc in enumerate(SIDES)
        ])
        self.vertical = both(lambda ch: [
            (
                spot.has(dr, 0),
                spot.has(-dr, 0),
                lambda k=k, dr=dr: remote(stack.at[ch, k], vbuf.at[ch, k], upright, (ch, k), spot.at(dr, 0)),
            )
            for k, dr in enumerate(SIDES)
        ])
        half = spot.half
        self.relay = Relay(
            spot,
            lambda row: accum.at[:, pl.ds(3 - 3 * half, 1), pl.ds(H + row, SLICE)],
            lambda row: mbuf.at[:, 1 - half, :, pl.ds(row, SLICE)],
            held, first, second,
        )

    def begin(self):
        self.corners[0].start()
        self.corners[1].start()

    def aside(self):
        self.relay.start()
        self.middle[0].start()
        self.middle[1].start()

    def turn(self, ch):
        stack, cbuf = self.stack, self.cbuf
        for k, side in enumerate(SIDES):
            stack[ch, k] = self.accum[ch, 1:3, part(OUTER_ROWS[side])]
        self.corners[ch].wait_recv()
        for (_, received, _), (k, n) in zip(self.corners[ch].entries, FOUR):

            @pl.when(received)
            def _():
                plane = INNER_PLANES[SIDES[n]][0] - 1
                stack[ch, k, plane] = stack[ch, k, plane] + cbuf[ch, 2 * k + n, 0]

        self.vertical[ch].start()
        self.across[ch].start()

    def end(self, ch, add):
        spot = self.spot
        self.middle[ch].wait_recv()
        if ch == 0:
            self.relay.wait_recv()
        for n, dc in enumerate(SIDES):

            @pl.when(spot.has(0, -dc))
            def _():
                add(self.mbuf.at[ch, n], (H, F), INNER_PLANES[dc])

        self.vertical[ch].wait_recv()
        for k, dr in enumerate(SIDES):

            @pl.when(spot.has(-dr, 0))
            def _():
                add(self.vbuf.at[ch, k], INNER_ROWS[dr], (1, 2))

        self.across[ch].wait_recv()
        for (_, received, _), (k, n) in zip(self.across[ch].entries, FOUR):

            @pl.when(received)
            def _():
                add(self.fbuf.at[ch, 2 * k + n], INNER_ROWS[SIDES[k]], INNER_PLANES[SIDES[n]])

    def close(self):
        for ch in range(2):
            for transfers in (self.corners[ch], self.across[ch], self.middle[ch], self.vertical[ch]):
                transfers.wait_send()
        self.relay.wait_send()


def mid_kernel(accum, old, frame, cbuf, mbuf, vbuf, fbuf, stack, held, held2, *sems):
    spot = Spot()
    greet(spot.peers())
    sems = pairs(sems)
    fold = Fold(spot, accum, cbuf, mbuf, vbuf, fbuf, stack, held, *sems[:6])
    halo = Halo(spot, frame, held2, *sems[6:])
    fold.begin()
    fold.aside()
    fold.turn(0)
    fold.turn(1)
    fold.relay.turn()
    clear_edges(spot.row, spot.col, frame)
    frame[:, 1:3, H : H + F] = old[:, 1:3, H : H + F] + accum[:, 1:3, H : H + F]
    for ch in range(2):

        def add(buf, rows, planes):
            where = (ch, part(planes), part(rows))
            frame[where] = frame[where] + buf[...]

        fold.end(ch, add)
        halo.begin(ch)
    halo.aside()
    halo.end()
    fold.close()


def held_buffer():
    return pltpu.VMEM((2, 1, SLICE, H), jnp.float32)


def fold_buffers():
    f32 = jnp.float32
    return [
        pltpu.VMEM((2, 4, 1, H, H), f32),
        pltpu.VMEM((2, 2, 1, F, H), f32),
        pltpu.VMEM((2, 2, 2, H, H), f32),
        pltpu.VMEM((2, 4, 1, H, H), f32),
        pltpu.VMEM((2, 2, 2, H, H), f32),
        held_buffer(),
    ]


def exchange_sems():
    dma = pltpu.SemaphoreType.DMA
    shapes = ((2, 2), (2, 2), (2, 4), (2, 4), (SEAM,), (SEAM,))
    return [dma(shape) for shape in shapes for _ in range(2)]


CHUNK1 = 64
CHUNK2 = 16
COLORS = (("x", "y"), ("y", "x"))


def last_kernel(accum, old, g, probe_re, probe_im, out_re, out_im, out, cbuf, mbuf, vbuf, fbuf, stack, held, *rest):
    exchange, rest = rest[:12], rest[12:]
    r0, w0, r1, w1, r2, w2, r3, w4, s0, q0, s1, q1, s2, q2, s3, q3, s4, q4, s5, q5, s6, q6 = rest
    spot = Spot()
    sy, sx = lax.axis_index("sy"), lax.axis_index("sx")
    here = {
        "y": lax.div(sy, 4),
        "x": lax.div(lax.rem(sx, 8), 2),
        "z": lax.div(sx, 8) * 4 + lax.rem(sy, 4),
        "core": lax.rem(sx, 2),
    }
    size = {"x": 4, "y": 4, "z": 8, "core": 2}
    rate = PROBE_GAIN / (8 * math.sqrt(ROWS * COLS))

    def place(axis, step):
        there = dict(here)
        there[axis] = lax.rem(here[axis] + step, size[axis])
        device = (
            there["y"] * 4 + lax.rem(there["z"], 4),
            lax.div(there["z"], 4) * 8 + there["x"] * 2 + there["core"],
        )
        return there[axis], device

    def send(src, dst, ss, rs, device):
        copy = pltpu.make_async_remote_copy(
            src_ref=src, dst_ref=dst, send_sem=ss, recv_sem=rs, device_id=device, device_id_type=MESH
        )
        copy.start()
        return copy

    fold = Fold(spot, accum, cbuf, mbuf, vbuf, fbuf, stack, held, *pairs(exchange))
    yes = sy >= 0
    greet(
        spot.peers()
        + [(yes, place(axis, step)[1]) for axis in ("core", "x", "y", "z") for step in range(1, size[axis])]
    )

    core = here["core"]
    other, partner = place("core", 1)
    mine = pl.ds(pl.multiple_of(core * 512, 512), 512)
    theirs = pl.ds(pl.multiple_of(other * 512, 512), 512)
    first_copy = send(g.at[theirs], r0, s0, q0, partner)
    first_copy.wait()
    w0[...] = g[mine] + r0[...]

    copies = []
    for c, (first, second) in enumerate(COLORS):
        for step in (1, 2, 3):
            index, device = place(first, step)
            source = w0.at[pl.ds(pl.multiple_of(c * 256 + index * CHUNK1, CHUNK1), CHUNK1)]
            copies.append(send(source, r1.at[c, step - 1], s1.at[c, step - 1], q1.at[c, step - 1], device))
    fold.begin()
    for copy in copies:
        copy.wait()
    for c, (first, second) in enumerate(COLORS):
        own = w0[pl.ds(pl.multiple_of(c * 256 + here[first] * CHUNK1, CHUNK1), CHUNK1)]
        w1[c] = (own + r1[c, 0]) + (r1[c, 1] + r1[c, 2])

    copies = []
    for c, (first, second) in enumerate(COLORS):
        for step in (1, 2, 3):
            index, device = place(second, step)
            source = w1.at[c, pl.ds(pl.multiple_of(index * CHUNK2, CHUNK2), CHUNK2)]
            copies.append(send(source, r2.at[c, step - 1], s2.at[c, step - 1], q2.at[c, step - 1], device))
    for copy in copies:
        copy.wait()
    for c, (first, second) in enumerate(COLORS):
        own = w1[c, pl.ds(pl.multiple_of(here[second] * CHUNK2, CHUNK2), CHUNK2)]
        w2[c] = (own + r2[c, 0]) + (r2[c, 1] + r2[c, 2])

    copies = []
    for c in range(2):
        for step in range(1, 8):
            index, device = place("z", step)
            copies.append(send(w2.at[c], r3.at[c, here["z"]], s3.at[c, step - 1], q3.at[c, step - 1], device))
    for c in range(2):
        r3[c, here["z"]] = w2[c]
    fold.turn(0)
    fold.turn(1)
    fold.aside()
    fold.relay.turn()
    outs = (out_re, out_im)
    for channel, tile in enumerate(outs):
        for n in range(2):
            tile[:, n * H : (n + 1) * H] = old[channel, 1 + n, H : H + F] + accum[channel, 1 + n, H : H + F]

    for copy in copies:
        copy.wait()
    for c, (first, second) in enumerate(COLORS):
        total = ((r3[c, 0] + r3[c, 1]) + (r3[c, 2] + r3[c, 3])) + ((r3[c, 4] + r3[c, 5]) + (r3[c, 6] + r3[c, 7]))
        start = c * 256 + here[first] * CHUNK1 + here[second] * CHUNK2
        spots = pl.ds(pl.multiple_of(start, CHUNK2), CHUNK2)
        base = jnp.where(core == 0, probe_re[spots], probe_im[spots])
        w4[c, pl.ds(pl.multiple_of(here[second] * CHUNK2, CHUNK2), CHUNK2)] = base + rate * total

    copies = []
    for c, (first, second) in enumerate(COLORS):
        spot = w4.at[c, pl.ds(pl.multiple_of(here[second] * CHUNK2, CHUNK2), CHUNK2)]
        for step in (1, 2, 3):
            copies.append(send(spot, spot, s4.at[c, step - 1], q4.at[c, step - 1], place(second, step)[1]))
    for copy in copies:
        copy.wait()

    copies = []
    for c, (first, second) in enumerate(COLORS):
        start = core * 512 + c * 256 + here[first] * CHUNK1
        spot = out.at[pl.ds(pl.multiple_of(start, CHUNK1), CHUNK1)]
        for step in (1, 2, 3):
            copies.append(send(w4.at[c], spot, s5.at[c, step - 1], q5.at[c, step - 1], place(first, step)[1]))
    for c, (first, second) in enumerate(COLORS):
        start = core * 512 + c * 256 + here[first] * CHUNK1
        out[pl.ds(pl.multiple_of(start, CHUNK1), CHUNK1)] = w4[c]
    for copy in copies:
        copy.wait()

    last_copy = send(out.at[mine], out.at[mine], s6, q6, partner)
    for ch, tile in enumerate(outs):

        def add(buf, rows, planes):
            for n in range(planes[1]):
                where = (pl.ds(rows[0] - H, rows[1]), pl.ds((planes[0] - 1 + n) * H, H))
                tile[where] = tile[where] + buf[n]

        fold.end(ch, add)
    fold.close()
    last_copy.wait()


def write_kernel(a, b, flat, out_a, out_b, out_c, out_d):
    out_a[...] = a[...]
    out_b[...] = b[...]
    for m in range(2):
        out_c[m] = flat[m * F : (m + 1) * F]
        out_d[m] = flat[(2 + m) * F : (3 + m) * F]


def work_kernel(batch, order, offsets, frame, probe_re, probe_im, amps, left, back_left, right, back_right, *rest):
    if batch == 0:
        accum, grad, patch, fields, halves, amp, amp_sem = rest
        grad_in = None
    else:
        grad_in, accum, grad, patch, fields, halves, amp, amp_sem = rest
    size = 4
    loads = []
    for j in range(size):
        p = order[batch * size + j]
        load = pltpu.make_async_copy(amps.at[p], amp.at[j], amp_sem.at[j])
        load.start()
        loads.append(load)

    power = jnp.max(
        probe_re[0] * probe_re[0]
        + probe_im[0] * probe_im[0]
        + (probe_re[1] * probe_re[1] + probe_im[1] * probe_im[1])
    )
    scale = OBJECT_RATE / jnp.full((8, 128), power, jnp.float32)[0:1, 0:1]
    accum[...] = jnp.zeros_like(accum)
    for j in range(size):
        p = order[batch * size + j]
        top = offsets[p, 0] + H
        shift = offsets[p, 1] + H
        for ch in range(2):
            rows = jnp.concatenate([frame[ch, n, pl.ds(top, F), :] for n in range(4)], axis=1)
            patch[j, ch] = pltpu.roll(rows, lax.rem(E - shift, E), 1)[:, :F]
        re, im = patch[j, 0], patch[j, 1]
        for m in range(2):
            at = pl.ds((2 * j + m) * F, F)
            fields[0:F, at] = (probe_re[m] * re - probe_im[m] * im).astype(jnp.bfloat16)
            fields[F : 2 * F, at] = (probe_re[m] * im + probe_im[m] * re).astype(jnp.bfloat16)
    for n in range(2 * size):
        half = jnp.dot(left[...], fields[0 : 2 * F, n * F : (n + 1) * F], preferred_element_type=jnp.float32)
        halves[n * F : (n + 1) * F, 0:F] = half[0:F].astype(jnp.bfloat16)
        halves[n * F : (n + 1) * F, F : 2 * F] = half[F:].astype(jnp.bfloat16)
    for j in range(size):
        far = jnp.dot(halves[2 * j * F : 2 * (j + 1) * F, :], right[...], preferred_element_type=jnp.float32)
        squares = far * far
        intensity = (squares[0:F, 0:F] + squares[0:F, F:]) + (squares[F:, 0:F] + squares[F:, F:])
        loads[j].wait()
        ratio = amp[j] * lax.rsqrt(jnp.maximum(intensity, 1.0))
        for m in range(2):
            at = (2 * j + m) * F
            fields[2 * F : 3 * F, at : at + F] = (far[m * F : (m + 1) * F, 0:F] * ratio).astype(jnp.bfloat16)
            fields[3 * F : 4 * F, at : at + F] = (far[m * F : (m + 1) * F, F:] * ratio).astype(jnp.bfloat16)
    for n in range(2 * size):
        half = jnp.dot(back_left[...], fields[2 * F :, n * F : (n + 1) * F], preferred_element_type=jnp.float32)
        halves[n * F : (n + 1) * F, 0:F] = half[0:F].astype(jnp.bfloat16)
        halves[n * F : (n + 1) * F, F : 2 * F] = half[F:].astype(jnp.bfloat16)
    for j in range(size):
        p = order[batch * size + j]
        top = offsets[p, 0] + H
        shift = offsets[p, 1] + H
        back = jnp.dot(halves[2 * j * F : 2 * (j + 1) * F, :], back_right[...], preferred_element_type=jnp.float32)
        re, im = patch[j, 0], patch[j, 1]
        terms = [None, None]
        for m in range(2):
            at = (2 * j + m) * F
            d_re = back[m * F : (m + 1) * F, 0:F] - fields[0:F, at : at + F].astype(jnp.float32)
            d_im = back[m * F : (m + 1) * F, F:] - fields[F : 2 * F, at : at + F].astype(jnp.float32)
            o_re = probe_re[m] * d_re + probe_im[m] * d_im
            o_im = probe_re[m] * d_im - probe_im[m] * d_re
            g_re = re * d_re + im * d_im
            g_im = re * d_im - im * d_re
            if m == 0:
                terms = [o_re, o_im]
            else:
                terms = [terms[0] + o_re, terms[1] + o_im]
            for ch, g in enumerate((g_re, g_im)):
                if j == 0:
                    grad[ch, m] = g if grad_in is None else grad_in[ch, m] + g
                else:
                    grad[ch, m] = grad[ch, m] + g
        for ch in range(2):
            wide = jnp.concatenate([terms[ch] * scale, jnp.zeros((F, F), jnp.float32)], axis=1)
            wide = pltpu.roll(wide, shift, 1)
            for n in range(4):
                accum[ch, n, pl.ds(top, F), :] += wide[:, n * H : (n + 1) * H]


def local(object_re, object_im, probe_re, probe_im, amplitudes, offsets, visit_order):
    f32 = jnp.float32
    amps = amplitudes.reshape(8, F, F)
    offs = offsets.reshape(8, 2)
    order = visit_order.reshape(8)
    tables = dft_operands()
    frame_shape = jax.ShapeDtypeStruct((2, 4, E, H), f32)
    grad_shape = jax.ShapeDtypeStruct((2, 2, F, F), f32)
    limit = 60 * 1024 * 1024

    def comm(kernel, outs, scratch, ident, n_in):
        return pl.pallas_call(
            kernel,
            out_shape=outs,
            in_specs=[VMEM] * n_in,
            out_specs=[VMEM] * len(outs) if isinstance(outs, list) else VMEM,
            scratch_shapes=scratch,
            compiler_params=pltpu.CompilerParams(
                collective_id=ident, has_side_effects=True, vmem_limit_bytes=limit
            ),
        )

    dma = pltpu.SemaphoreType.DMA

    def work(batch, frame, grad):
        ins = [order, offs, frame, probe_re, probe_im, amps, *tables]
        specs = [SMEM, SMEM, VMEM, VMEM, VMEM, ANY] + [VMEM] * 4
        if grad is not None:
            ins.append(grad)
            specs.append(VMEM)
        return pl.pallas_call(
            functools.partial(work_kernel, batch),
            out_shape=[frame_shape, grad_shape],
            in_specs=specs,
            out_specs=[VMEM, VMEM],
            scratch_shapes=[
                pltpu.VMEM((4, 2, F, F), f32),
                pltpu.VMEM((4 * F, 8 * F), jnp.bfloat16),
                pltpu.VMEM((8 * F, 2 * F), jnp.bfloat16),
                pltpu.VMEM((4, F, F), f32),
                dma((4,)),
            ],
            compiler_params=pltpu.CompilerParams(vmem_limit_bytes=limit),
            cost_estimate=pl.CostEstimate(flops=4_300_000_000, bytes_accessed=10_000_000, transcendentals=262144),
        )(*ins)

    frame = comm(halo_kernel, frame_shape, [held_buffer()] + exchange_sems(), 0, 2)(object_re, object_im)
    accum, grad = work(0, frame, None)
    frame = comm(mid_kernel, frame_shape, fold_buffers() + [held_buffer()] + exchange_sems() + exchange_sems(), 1, 2)(accum, frame)
    accum, grad = work(1, frame, grad)
    tile_shape = jax.ShapeDtypeStruct((F, F), f32)
    out_re, out_im, flat = comm(
        last_kernel,
        [tile_shape, tile_shape, jax.ShapeDtypeStruct((1024, F), f32)],
        fold_buffers()
        + exchange_sems()
        + [
            pltpu.VMEM((512, F), f32),
            pltpu.VMEM((512, F), f32),
            pltpu.VMEM((2, 3, CHUNK1, F), f32),
            pltpu.VMEM((2, CHUNK1, F), f32),
            pltpu.VMEM((2, 3, CHUNK2, F), f32),
            pltpu.VMEM((2, CHUNK2, F), f32),
            pltpu.VMEM((2, 8, CHUNK2, F), f32),
            pltpu.VMEM((2, CHUNK1, F), f32),
            dma, dma,
            dma((2, 3)), dma((2, 3)),
            dma((2, 3)), dma((2, 3)),
            dma((2, 7)), dma((2, 7)),
            dma((2, 3)), dma((2, 3)),
            dma((2, 3)), dma((2, 3)),
            dma, dma,
        ],
        2,
        5,
    )(accum, frame, grad.reshape(1024, F), probe_re.reshape(512, F), probe_im.reshape(512, F))
    probe_shape = jax.ShapeDtypeStruct((2, F, F), f32)
    return tuple(
        pl.pallas_call(
            write_kernel,
            out_shape=[tile_shape, tile_shape, probe_shape, probe_shape],
            in_specs=[VMEM] * 3,
            out_specs=[VMEM] * 4,
        )(out_re, out_im, flat)
    )


def solution(mesh):
    return jax.shard_map(
        local,
        mesh=mesh,
        in_specs=(
            P("sy", "sx"),
            P("sy", "sx"),
            P(),
            P(),
            P("sy", "sx", None, None, None),
            P("sy", "sx", None, None),
            P("sy", "sx", None),
        ),
        out_specs=(P("sy", "sx"), P("sy", "sx"), P(), P()),
        check_vma=False,
    )
```

```python
import math

import numpy as np

import jax
import jax.numpy as jnp
from jax import lax
from jax.experimental import pallas as pl
from jax.experimental.pallas import tpu as pltpu
from jax.sharding import PartitionSpec as P

MESH = pl.DeviceIdType.MESH
BATCHES = 2
OBJECT_RATE = 0.25
PROBE_GAIN = 4.0
F = 256
H = 128
E = F + 2 * H
ROWS = 16
COLS = 16
SEAM = 8
VMEM = pl.BlockSpec(memory_space=pltpu.VMEM)
SMEM = pl.BlockSpec(memory_space=pltpu.SMEM)
ANY = pl.BlockSpec(memory_space=pl.ANY)
TILE_ROWS = {-1: (H, H), 0: (H, F), 1: (F, H)}
TILE_PLANES = {-1: (1, 1), 0: (1, 2), 1: (2, 1)}
OUTER_ROWS = {-1: (0, H), 0: (H, F), 1: (H + F, H)}
OUTER_PLANES = {-1: (0, 1), 0: (1, 2), 1: (3, 1)}
FRAME_ROWS = {-1: (H + F, H), 0: (H, F), 1: (0, H)}
FRAME_PLANES = {-1: (3, 1), 0: (1, 2), 1: (0, 1)}
INNER_ROWS = {-1: (F, H), 0: (H, F), 1: (H, H)}
INNER_PLANES = {-1: (2, 1), 0: (1, 2), 1: (1, 1)}


def table(frame_size):
    ramp = np.arange(frame_size, dtype=np.int64)
    product = (ramp[:, None] * ramp[None, :]) % frame_size
    angle = np.float32(2.0 * math.pi / frame_size) * product.astype(np.float32)
    scale = np.float32(1.0 / math.sqrt(frame_size))
    return np.cos(angle) * scale, -np.sin(angle) * scale


def dft_operands():
    re, im = table(F)
    left = np.block([[re, -im], [im, re]])
    right = np.block([[re, im], [-im, re]])
    return [jnp.asarray(m, jnp.float32).astype(jnp.bfloat16) for m in (left, right)]


def part(pair):
    return pl.ds(pair[0], pair[1])


def inside(row, col):
    return (row >= 0) & (row < ROWS) & (col >= 0) & (col < COLS)


def greet(peers, meanwhile):
    barrier = pltpu.get_barrier_semaphore()
    count = jnp.int32(0)
    for there, device in peers:

        @pl.when(there)
        def _():
            pl.semaphore_signal(barrier, inc=1, device_id=device, device_id_type=MESH)

        count = count + there.astype(jnp.int32)
    meanwhile()
    pl.semaphore_wait(barrier, count)


class Spot:
    def __init__(self):
        self.row, self.col = lax.axis_index("sy"), lax.axis_index("sx")
        self.half = lax.div(self.col, SEAM)
        self.seat = lax.rem(self.col, SEAM)
        self.seam = (self.col == SEAM - 1) | (self.col == SEAM)
        self.edge = (self.row, SEAM - 1 + self.half)
        self.beyond = (self.row, SEAM - self.half)

    def at(self, dr, dc):
        return (self.row + dr, self.col + dc)

    def has(self, dr, dc):
        return inside(self.row + dr, self.col + dc)

    def far(self, dc):
        return self.col == (SEAM - 1 if dc > 0 else SEAM)

    def peers(self):
        near = [(self.has(dr, dc), self.at(dr, dc)) for dr, dc in ((-1, 0), (1, 0), (0, -1), (0, 1))]
        diagonal = [
            (self.has(dr, dc) & self.far(dc), self.at(dr, dc)) for dr in (-1, 1) for dc in (-1, 1)
        ]
        row, col = self.row, self.col
        relays = [
            (self.seam & (col != c) & (jnp.abs(col - c) != 1), (row, jnp.int32(c))) for c in range(COLS)
        ]
        edges = [(~self.seam & (jnp.abs(col - c) != 1), (row, jnp.int32(c))) for c in (SEAM - 1, SEAM)]
        return near + diagonal + relays[: SEAM - 1] + relays[SEAM + 1 :] + [
            (self.seam & (there), device) for there, device in relays[SEAM - 1 : SEAM + 1]
        ] + edges


def remote(src, dst, sems, at, device):
    return pltpu.make_async_remote_copy(
        src_ref=src,
        dst_ref=dst,
        send_sem=sems[0].at[at],
        recv_sem=sems[1].at[at],
        device_id=device,
        device_id_type=MESH,
    )


class Transfers:
    def __init__(self, entries):
        self.entries = entries

    def start(self):
        for sent, received, build in self.entries:

            @pl.when(sent)
            def _():
                build().start()

    def wait_recv(self):
        for sent, received, build in self.entries:

            @pl.when(received)
            def _():
                build().wait_recv()

    def wait_send(self):
        for sent, received, build in self.entries:

            @pl.when(sent)
            def _():
                build().wait_send()


SIDES = (-1, 1)


def clear_edges(row, col, frame):
    @pl.when(row == 0)
    def _():
        frame[:, :, 0:H, :] = jnp.zeros((2, 4, H, H), jnp.float32)

    @pl.when(row == ROWS - 1)
    def _():
        frame[:, :, H + F : E, :] = jnp.zeros((2, 4, H, H), jnp.float32)

    @pl.when(col == 0)
    def _():
        frame[:, 0] = jnp.zeros((2, E, H), jnp.float32)

    @pl.when(col == COLS - 1)
    def _():
        frame[:, 3] = jnp.zeros((2, E, H), jnp.float32)


FOUR = [(k, n) for k in range(2) for n in range(2)]
SLICE = F // SEAM


class Relay:
    def __init__(self, spot, source, target, held, first, second):
        self.spot, self.source, self.target, self.held = spot, source, target, held
        self.first, self.second = first, second

    def out(self, q):
        spot = self.spot
        device = (spot.row, spot.half * SEAM + q)
        return remote(self.source(q * SLICE), self.held, self.first, q, device)

    def arrive(self):
        return pltpu.make_async_remote_copy(
            src_ref=self.held, dst_ref=self.held, send_sem=self.first[0].at[0],
            recv_sem=self.first[1].at[self.spot.seat], device_id=self.spot.edge, device_id_type=MESH,
        )

    def on(self, q, src):
        return remote(src, self.target(pl.multiple_of(q * SLICE, SLICE)), self.second, q, self.spot.beyond)

    def start(self):
        spot = self.spot
        for q in range(SEAM):

            @pl.when(spot.seam & (spot.seat != q))
            def _():
                self.out(q).start()

        for half, q in ((0, SEAM - 1), (1, 0)):

            @pl.when(spot.seam & (spot.half == half))
            def _():
                self.on(q, self.source(q * SLICE)).start()

    def turn(self):
        @pl.when(~self.spot.seam)
        def _():
            self.arrive().wait_recv()
            self.on(self.spot.seat, self.held).start()

    def wait_recv(self):
        @pl.when(self.spot.seam)
        def _():
            for q in range(SEAM):
                self.on(q, self.held).wait_recv()

    def wait_send(self):
        spot = self.spot

        @pl.when(~spot.seam)
        def _():
            self.on(spot.seat, self.held).wait_send()

        for q in range(SEAM):

            @pl.when(spot.seam & (spot.seat != q))
            def _():
                self.out(q).wait_send()

        for half, q in ((0, SEAM - 1), (1, 0)):

            @pl.when(spot.seam & (spot.half == half))
            def _():
                self.on(q, self.held).wait_send()


class Halo:
    def __init__(self, spot, frame, held, upright, level, corner, seam, first, second):
        self.spot, self.frame = spot, frame

        def strip(ch, dr, planes, rows_from, to_rows, to_planes, sems, k, device):
            c = pl.ds(ch, 1)
            return lambda: remote(
                frame.at[c, part(planes), part(rows_from)], frame.at[c, part(to_planes), part(to_rows)], sems, (ch, k), device
            )

        def both(make):
            return [Transfers(make(ch)) for ch in range(2)]

        self.vertical = both(lambda ch: [
            (
                spot.has(dr, 0),
                spot.has(-dr, 0),
                strip(ch, dr, (1, 2), TILE_ROWS[dr], FRAME_ROWS[dr], (1, 2), upright, k, spot.at(dr, 0)),
            )
            for k, dr in enumerate(SIDES)
        ])
        self.across = both(lambda ch: [
            (
                spot.has(dr, dc) & spot.far(dc),
                spot.has(-dr, -dc) & spot.far(-dc),
                strip(ch, dr, TILE_PLANES[dc], TILE_ROWS[dr], FRAME_ROWS[dr], FRAME_PLANES[dc], seam, 2 * k + n, spot.at(dr, dc)),
            )
            for k, dr in enumerate(SIDES)
            for n, dc in enumerate(SIDES)
        ])
        self.middle = both(lambda ch: [
            (
                spot.has(0, dc) & ~spot.far(dc),
                spot.has(0, -dc) & ~spot.far(-dc),
                strip(ch, 0, TILE_PLANES[dc], (H, F), (H, F), FRAME_PLANES[dc], level, n, spot.at(0, dc)),
            )
            for n, dc in enumerate(SIDES)
        ])
        self.corners = both(lambda ch: [
            (
                spot.has(side, 0) & spot.has(0, dc) & ~spot.far(dc),
                spot.has(side, 0) & spot.has(0, -dc) & ~spot.far(-dc),
                strip(ch, 0, TILE_PLANES[dc], OUTER_ROWS[side], OUTER_ROWS[side], FRAME_PLANES[dc], corner, 2 * k + n, spot.at(0, dc)),
            )
            for k, side in enumerate(SIDES)
            for n, dc in enumerate(SIDES)
        ])
        half = spot.half
        self.relay = Relay(
            spot,
            lambda row: frame.at[:, pl.ds(2 - half, 1), pl.ds(H + row, SLICE)],
            lambda row: frame.at[:, pl.ds(3 * half, 1), pl.ds(H + row, SLICE)],
            held, first, second,
        )

    def begin(self, ch):
        self.vertical[ch].start()
        self.across[ch].start()

    def aside(self):
        self.relay.start()
        self.middle[0].start()
        self.middle[1].start()
        self.relay.turn()

    def end(self):
        for ch in range(2):
            self.vertical[ch].wait_recv()
            self.corners[ch].start()
        for ch in range(2):
            self.middle[ch].wait_recv()
        self.relay.wait_recv()
        for ch in range(2):
            for transfers in (self.across[ch], self.corners[ch]):
                transfers.wait_recv()
        for ch in range(2):
            for transfers in (self.vertical[ch], self.middle[ch], self.across[ch], self.corners[ch]):
                transfers.wait_send()
        self.relay.wait_send()


def pairs(sems):
    return [(sems[i], sems[i + 1]) for i in range(0, len(sems), 2)]


class Fold:
    def __init__(self, spot, accum, cbuf, mbuf, vbuf, fbuf, stack, held, upright, level, corner, seam, first, second):
        self.spot, self.accum, self.stack = spot, accum, stack
        self.cbuf, self.mbuf, self.vbuf, self.fbuf = cbuf, mbuf, vbuf, fbuf

        def strip(ch, planes, rows, buf, sems, k, device):
            return lambda: remote(accum.at[ch, part(planes), part(rows)], buf.at[ch, k], sems, (ch, k), device)

        def both(make):
            return [Transfers(make(ch)) for ch in range(2)]

        self.corners = both(lambda ch: [
            (
                spot.has(side, 0) & spot.has(0, dc) & ~spot.far(dc),
                spot.has(side, 0) & spot.has(0, -dc) & ~spot.far(-dc),
                strip(ch, OUTER_PLANES[dc], OUTER_ROWS[side], cbuf, corner, 2 * k + n, spot.at(0, dc)),
            )
            for k, side in enumerate(SIDES)
            for n, dc in enumerate(SIDES)
        ])
        self.across = both(lambda ch: [
            (
                spot.has(dr, dc) & spot.far(dc),
                spot.has(-dr, -dc) & spot.far(-dc),
                strip(ch, OUTER_PLANES[dc], OUTER_ROWS[dr], fbuf, seam, 2 * k + n, spot.at(dr, dc)),
            )
            for k, dr in enumerate(SIDES)
            for n, dc in enumerate(SIDES)
        ])
        self.middle = both(lambda ch: [
            (
                spot.has(0, dc) & ~spot.far(dc),
                spot.has(0, -dc) & ~spot.far(-dc),
                strip(ch, OUTER_PLANES[dc], (H, F), mbuf, level, n, spot.at(0, dc)),
            )
            for n, dc in enumerate(SIDES)
        ])
        self.vertical = both(lambda ch: [
            (
                spot.has(dr, 0),
                spot.has(-dr, 0),
                lambda k=k, dr=dr: remote(stack.at[ch, k], vbuf.at[ch, k], upright, (ch, k), spot.at(dr, 0)),
            )
            for k, dr in enumerate(SIDES)
        ])
        half = spot.half
        self.relay = Relay(
            spot,
            lambda row: accum.at[:, pl.ds(3 - 3 * half, 1), pl.ds(H + row, SLICE)],
            lambda row: mbuf.at[:, 1 - half, :, pl.ds(row, SLICE)],
            held, first, second,
        )

    def begin(self):
        self.corners[0].start()
        self.corners[1].start()

    def aside(self):
        self.relay.start()
        self.middle[0].start()
        self.middle[1].start()

    def turn(self, ch):
        stack, cbuf = self.stack, self.cbuf
        for k, side in enumerate(SIDES):
            stack[ch, k] = self.accum[ch, 1:3, part(OUTER_ROWS[side])]
        self.corners[ch].wait_recv()
        for (_, received, _), (k, n) in zip(self.corners[ch].entries, FOUR):

            @pl.when(received)
            def _():
                plane = INNER_PLANES[SIDES[n]][0] - 1
                stack[ch, k, plane] = stack[ch, k, plane] + cbuf[ch, 2 * k + n, 0]

        self.vertical[ch].start()
        self.across[ch].start()

    def end(self, ch, add):
        spot = self.spot
        self.middle[ch].wait_recv()
        if ch == 0:
            self.relay.wait_recv()
        for n, dc in enumerate(SIDES):

            @pl.when(spot.has(0, -dc))
            def _():
                add(self.mbuf.at[ch, n], (H, F), INNER_PLANES[dc])

        self.vertical[ch].wait_recv()
        for k, dr in enumerate(SIDES):

            @pl.when(spot.has(-dr, 0))
            def _():
                add(self.vbuf.at[ch, k], INNER_ROWS[dr], (1, 2))

        self.across[ch].wait_recv()
        for (_, received, _), (k, n) in zip(self.across[ch].entries, FOUR):

            @pl.when(received)
            def _():
                add(self.fbuf.at[ch, 2 * k + n], INNER_ROWS[SIDES[k]], INNER_PLANES[SIDES[n]])

    def close(self):
        for ch in range(2):
            for transfers in (self.corners[ch], self.across[ch], self.middle[ch], self.vertical[ch]):
                transfers.wait_send()
        self.relay.wait_send()


def renew(spot, fold, halo, accum, frame):
    fold.begin()
    fold.aside()
    fold.turn(0)
    fold.turn(1)
    fold.relay.turn()
    frame[:, 1:3, H : H + F] = frame[:, 1:3, H : H + F] + accum[:, 1:3, H : H + F]
    for ch in range(2):

        def add(buf, rows, planes):
            where = (ch, part(planes), part(rows))
            frame[where] = frame[where] + buf[...]

        fold.end(ch, add)
        halo.begin(ch)
    halo.aside()
    halo.end()
    fold.close()


def held_buffer():
    return pltpu.VMEM((2, 1, SLICE, H), jnp.float32)


def fold_buffers():
    f32 = jnp.float32
    return [
        pltpu.VMEM((2, 4, 1, H, H), f32),
        pltpu.VMEM((2, 2, 1, F, H), f32),
        pltpu.VMEM((2, 2, 2, H, H), f32),
        pltpu.VMEM((2, 4, 1, H, H), f32),
        pltpu.VMEM((2, 2, 2, H, H), f32),
        held_buffer(),
    ]


def exchange_sems():
    dma = pltpu.SemaphoreType.DMA
    shapes = ((2, 2), (2, 2), (2, 4), (2, 4), (SEAM,), (SEAM,))
    return [dma(shape) for shape in shapes for _ in range(2)]


CHUNK1 = 64
CHUNK2 = 16
COLORS = (("x", "y"), ("y", "x"))


def torus():
    sy, sx = lax.axis_index("sy"), lax.axis_index("sx")
    here = {
        "y": lax.div(sy, 4),
        "x": lax.div(lax.rem(sx, 8), 2),
        "z": lax.div(sx, 8) * 4 + lax.rem(sy, 4),
        "core": lax.rem(sx, 2),
    }
    size = {"x": 4, "y": 4, "z": 8, "core": 2}

    def place(axis, step):
        there = dict(here)
        there[axis] = lax.rem(here[axis] + step, size[axis])
        device = (
            there["y"] * 4 + lax.rem(there["z"], 4),
            lax.div(there["z"], 4) * 8 + there["x"] * 2 + there["core"],
        )
        return there[axis], device

    return here, place


def finish_all(fold, accum, old, g, probe_re, probe_im, out_re, out_im, out, *rest):
    r0, w0, r1, w1, r2, w2, r3, w4, s0, q0, s1, q1, s2, q2, s3, q3, s4, q4, s5, q5, s6, q6 = rest
    here, place = torus()
    rate = PROBE_GAIN / (8 * math.sqrt(ROWS * COLS))

    def send(src, dst, ss, rs, device):
        copy = pltpu.make_async_remote_copy(
            src_ref=src, dst_ref=dst, send_sem=ss, recv_sem=rs, device_id=device, device_id_type=MESH
        )
        copy.start()
        return copy

    core = here["core"]
    other, partner = place("core", 1)
    mine = pl.ds(pl.multiple_of(core * 512, 512), 512)
    theirs = pl.ds(pl.multiple_of(other * 512, 512), 512)
    first_copy = send(g.at[theirs], r0, s0, q0, partner)
    first_copy.wait()
    w0[...] = g[mine] + r0[...]

    copies = []
    for c, (first, second) in enumerate(COLORS):
        for step in (1, 2, 3):
            index, device = place(first, step)
            source = w0.at[pl.ds(pl.multiple_of(c * 256 + index * CHUNK1, CHUNK1), CHUNK1)]
            copies.append(send(source, r1.at[c, step - 1], s1.at[c, step - 1], q1.at[c, step - 1], device))
    fold.begin()
    for copy in copies:
        copy.wait()
    for c, (first, second) in enumerate(COLORS):
        own = w0[pl.ds(pl.multiple_of(c * 256 + here[first] * CHUNK1, CHUNK1), CHUNK1)]
        w1[c] = (own + r1[c, 0]) + (r1[c, 1] + r1[c, 2])

    copies = []
    for c, (first, second) in enumerate(COLORS):
        for step in (1, 2, 3):
            index, device = place(second, step)
            source = w1.at[c, pl.ds(pl.multiple_of(index * CHUNK2, CHUNK2), CHUNK2)]
            copies.append(send(source, r2.at[c, step - 1], s2.at[c, step - 1], q2.at[c, step - 1], device))
    for copy in copies:
        copy.wait()
    for c, (first, second) in enumerate(COLORS):
        own = w1[c, pl.ds(pl.multiple_of(here[second] * CHUNK2, CHUNK2), CHUNK2)]
        w2[c] = (own + r2[c, 0]) + (r2[c, 1] + r2[c, 2])

    copies = []
    for c in range(2):
        for step in range(1, 8):
            index, device = place("z", step)
            copies.append(send(w2.at[c], r3.at[c, here["z"]], s3.at[c, step - 1], q3.at[c, step - 1], device))
    for c in range(2):
        r3[c, here["z"]] = w2[c]
    fold.turn(0)
    fold.turn(1)
    fold.aside()
    fold.relay.turn()
    outs = (out_re, out_im)
    for channel, tile in enumerate(outs):
        for n in range(2):
            tile[:, n * H : (n + 1) * H] = old[channel, 1 + n, H : H + F] + accum[channel, 1 + n, H : H + F]

    for copy in copies:
        copy.wait()
    for c, (first, second) in enumerate(COLORS):
        total = ((r3[c, 0] + r3[c, 1]) + (r3[c, 2] + r3[c, 3])) + ((r3[c, 4] + r3[c, 5]) + (r3[c, 6] + r3[c, 7]))
        start = c * 256 + here[first] * CHUNK1 + here[second] * CHUNK2
        own = pl.ds(pl.multiple_of(lax.rem(start, F), CHUNK2), CHUNK2)
        mode = lax.div(start, F)
        base = jnp.where(core == 0, probe_re[mode, own], probe_im[mode, own])
        w4[c, pl.ds(pl.multiple_of(here[second] * CHUNK2, CHUNK2), CHUNK2)] = base + rate * total

    copies = []
    for c, (first, second) in enumerate(COLORS):
        spot = w4.at[c, pl.ds(pl.multiple_of(here[second] * CHUNK2, CHUNK2), CHUNK2)]
        for step in (1, 2, 3):
            copies.append(send(spot, spot, s4.at[c, step - 1], q4.at[c, step - 1], place(second, step)[1]))
    for copy in copies:
        copy.wait()

    copies = []
    for c, (first, second) in enumerate(COLORS):
        start = core * 512 + c * 256 + here[first] * CHUNK1
        spot = out.at[pl.ds(pl.multiple_of(start, CHUNK1), CHUNK1)]
        for step in (1, 2, 3):
            copies.append(send(w4.at[c], spot, s5.at[c, step - 1], q5.at[c, step - 1], place(first, step)[1]))
    for c, (first, second) in enumerate(COLORS):
        start = core * 512 + c * 256 + here[first] * CHUNK1
        out[pl.ds(pl.multiple_of(start, CHUNK1), CHUNK1)] = w4[c]
    for copy in copies:
        copy.wait()

    last_copy = send(out.at[mine], out.at[mine], s6, q6, partner)
    for ch, tile in enumerate(outs):

        def add(buf, rows, planes):
            for n in range(planes[1]):
                where = (pl.ds(rows[0] - H, rows[1]), pl.ds((planes[0] - 1 + n) * H, H))
                tile[where] = tile[where] + buf[n]

        fold.end(ch, add)
    fold.close()
    last_copy.wait()


def write_kernel(a, b, flat, out_a, out_b, out_c, out_d):
    out_a[...] = a[...]
    out_b[...] = b[...]
    for m in range(2):
        out_c[m] = flat[m * F : (m + 1) * F]
        out_d[m] = flat[(2 + m) * F : (3 + m) * F]


def place_terms(batch, order, offsets, accum, padded):
    starts = []
    for j in range(4):
        starts.append(F - (offsets[order[batch * 4 + j], 0] + H))
    for ch in range(2):
        for n in range(4):
            for row in range(0, E, H):
                parts = [padded[j, ch, n, pl.ds(starts[j] + row, H), :] for j in range(4)]
                accum[ch, n, row : row + H, :] = (parts[0] + parts[1]) + (parts[2] + parts[3])


def work(batch, order, offsets, frame, probe_re, probe_im, amps, amp_ready, left, right, accum, grad, scale, padded, patch, fields, halves):
    back_left, back_right = right, left
    size = 4
    for j in range(size):
        p = order[batch * size + j]
        top = offsets[p, 0] + H
        shift = offsets[p, 1] + H
        for ch in range(2):
            rows = jnp.concatenate([frame[ch, n, pl.ds(top, F), :] for n in range(4)], axis=1)
            patch[j, ch] = pltpu.roll(rows, lax.rem(E - shift, E), 1)[:, :F]
        re, im = patch[j, 0], patch[j, 1]
        for m in range(2):
            at = pl.ds((2 * j + m) * F, F)
            fields[0:F, at] = (probe_re[m] * re - probe_im[m] * im).astype(jnp.bfloat16)
            fields[F : 2 * F, at] = (probe_re[m] * im + probe_im[m] * re).astype(jnp.bfloat16)
    for n in range(2 * size):
        half = jnp.dot(left[...], fields[0 : 2 * F, n * F : (n + 1) * F], preferred_element_type=jnp.float32)
        halves[n * F : (n + 1) * F, 0:F] = half[0:F].astype(jnp.bfloat16)
        halves[n * F : (n + 1) * F, F : 2 * F] = half[F:].astype(jnp.bfloat16)
    for j in range(size):
        far = jnp.dot(halves[2 * j * F : 2 * (j + 1) * F, :], right[...], preferred_element_type=jnp.float32)
        squares = far * far
        intensity = (squares[0:F, 0:F] + squares[0:F, F:]) + (squares[F:, 0:F] + squares[F:, F:])
        if j == 0:
            amp_ready()
        ratio = amps[order[batch * size + j]] * lax.rsqrt(jnp.maximum(intensity, 1.0))
        for m in range(2):
            at = (2 * j + m) * F
            fields[2 * F : 3 * F, at : at + F] = (far[m * F : (m + 1) * F, 0:F] * ratio).astype(jnp.bfloat16)
            fields[3 * F : 4 * F, at : at + F] = (far[m * F : (m + 1) * F, F:] * ratio).astype(jnp.bfloat16)
    for n in range(2 * size):
        half = jnp.dot(back_left[...], fields[2 * F :, n * F : (n + 1) * F], preferred_element_type=jnp.float32)
        halves[n * F : (n + 1) * F, 0:F] = half[0:F].astype(jnp.bfloat16)
        halves[n * F : (n + 1) * F, F : 2 * F] = half[F:].astype(jnp.bfloat16)
    for j in range(size):
        p = order[batch * size + j]
        top = offsets[p, 0] + H
        shift = offsets[p, 1] + H
        back = jnp.dot(halves[2 * j * F : 2 * (j + 1) * F, :], back_right[...], preferred_element_type=jnp.float32)
        re, im = patch[j, 0], patch[j, 1]
        terms = [None, None]
        for m in range(2):
            at = (2 * j + m) * F
            d_re = back[m * F : (m + 1) * F, 0:F] - fields[0:F, at : at + F].astype(jnp.float32)
            d_im = back[m * F : (m + 1) * F, F:] - fields[F : 2 * F, at : at + F].astype(jnp.float32)
            o_re = probe_re[m] * d_re + probe_im[m] * d_im
            o_im = probe_re[m] * d_im - probe_im[m] * d_re
            g_re = re * d_re + im * d_im
            g_im = re * d_im - im * d_re
            if m == 0:
                terms = [o_re, o_im]
            else:
                terms = [terms[0] + o_re, terms[1] + o_im]
            for ch, g in enumerate((g_re, g_im)):
                own = pl.ds((2 * ch + m) * F, F)
                if j == 0 and batch == 0:
                    grad[own] = g
                else:
                    grad[own] = grad[own] + g
        for ch in range(2):
            wide = jnp.concatenate([terms[ch] * scale[0:1, 0:1], jnp.zeros((F, F), jnp.float32)], axis=1)
            wide = pltpu.roll(wide, shift, 1)
            for n in range(4):
                padded[j, ch, n, F : 2 * F, :] = wide[:, n * H : (n + 1) * H]
    place_terms(batch, order, offsets, accum, padded)


def whole_kernel(order, offsets, re_ref, im_ref, probe_re_in, probe_im_in, amps_in, left_in, right_in, out_re, out_im, out, *scratch):
    frame, accum, probe_re, probe_im, amps, left, right, grad, scale, padded, patch, fields, halves, load_sem = scratch[:14]
    buffers, sems, rest = scratch[14:28], pairs(scratch[28:76]), scratch[76:]
    spot = Spot()
    loads = [
        pltpu.make_async_copy(source, target, load_sem.at[i])
        for i, (source, target) in enumerate(
            [(probe_re_in, probe_re), (probe_im_in, probe_im), (left_in, left), (right_in, right), (amps_in, amps)]
        )
    ]
    for load in loads:
        load.start()

    def meanwhile():
        for channel, source in enumerate((re_ref, im_ref)):
            for n in range(2):
                frame[channel, 1 + n, H : H + F] = source[:, n * H : (n + 1) * H]
        clear_edges(spot.row, spot.col, frame)

    here, place = torus()
    yes = spot.row >= 0
    size = {"core": 2, "x": 4, "y": 4, "z": 8}
    greet(
        spot.peers()
        + [(yes, place(axis, step)[1]) for axis in size for step in range(1, size[axis])],
        meanwhile,
    )
    halo = Halo(spot, frame, buffers[12], *sems[0:6])
    halo.begin(0)
    halo.begin(1)
    halo.aside()
    blank = jnp.zeros((F, H), jnp.float32)
    for j in range(4):
        for ch in range(2):
            for n in range(4):
                padded[j, ch, n, 0:F] = blank
                padded[j, ch, n, 2 * F : 3 * F] = blank
    for load in loads[:4]:
        load.wait()
    power = jnp.max(
        probe_re[0] * probe_re[0]
        + probe_im[0] * probe_im[0]
        + (probe_re[1] * probe_re[1] + probe_im[1] * probe_im[1]),
        keepdims=True,
    )
    scale[...] = jnp.broadcast_to(OBJECT_RATE / power, (8, H))
    halo.end()
    common = (left, right, accum, grad, scale, padded, patch, fields, halves)
    work(0, order, offsets, frame, probe_re, probe_im, amps, loads[4].wait, *common)
    fold = Fold(spot, accum, *buffers[0:6], *sems[6:12])
    halo = Halo(spot, frame, buffers[13], *sems[12:18])
    renew(spot, fold, halo, accum, frame)
    work(1, order, offsets, frame, probe_re, probe_im, amps, lambda: None, *common)
    fold = Fold(spot, accum, *buffers[6:12], *sems[18:24])
    finish_all(fold, accum, frame, grad, probe_re, probe_im, out_re, out_im, out, *rest)


def local(object_re, object_im, probe_re, probe_im, amplitudes, offsets, visit_order):
    f32, bf16 = jnp.float32, jnp.bfloat16
    left, right = dft_operands()
    dma = pltpu.SemaphoreType.DMA
    tile_shape = jax.ShapeDtypeStruct((F, F), f32)
    out_re, out_im, flat = pl.pallas_call(
        whole_kernel,
        out_shape=[tile_shape, tile_shape, jax.ShapeDtypeStruct((4 * F, F), f32)],
        in_specs=[SMEM, SMEM, VMEM, VMEM, ANY, ANY, ANY, ANY, ANY],
        out_specs=[VMEM] * 3,
        scratch_shapes=[
            pltpu.VMEM((2, 4, E, H), f32),
            pltpu.VMEM((2, 4, E, H), f32),
            pltpu.VMEM((2, F, F), f32),
            pltpu.VMEM((2, F, F), f32),
            pltpu.VMEM((8, F, F), f32),
            pltpu.VMEM((2 * F, 2 * F), bf16),
            pltpu.VMEM((2 * F, 2 * F), bf16),
            pltpu.VMEM((4 * F, F), f32),
            pltpu.VMEM((8, H), f32),
            pltpu.VMEM((4, 2, 4, 3 * F, H), f32),
            pltpu.VMEM((4, 2, F, F), f32),
            pltpu.VMEM((4 * F, 8 * F), bf16),
            pltpu.VMEM((8 * F, 2 * F), bf16),
            dma((5,)),
        ]
        + fold_buffers()
        + fold_buffers()
        + [held_buffer(), held_buffer()]
        + exchange_sems() * 4
        + [
            pltpu.VMEM((512, F), f32),
            pltpu.VMEM((512, F), f32),
            pltpu.VMEM((2, 3, CHUNK1, F), f32),
            pltpu.VMEM((2, CHUNK1, F), f32),
            pltpu.VMEM((2, 3, CHUNK2, F), f32),
            pltpu.VMEM((2, CHUNK2, F), f32),
            pltpu.VMEM((2, 8, CHUNK2, F), f32),
            pltpu.VMEM((2, CHUNK1, F), f32),
            dma, dma,
            dma((2, 3)), dma((2, 3)),
            dma((2, 3)), dma((2, 3)),
            dma((2, 7)), dma((2, 7)),
            dma((2, 3)), dma((2, 3)),
            dma((2, 3)), dma((2, 3)),
            dma, dma,
        ],
        compiler_params=pltpu.CompilerParams(
            collective_id=0, has_side_effects=True, vmem_limit_bytes=62 * 1024 * 1024
        ),
    )(
        visit_order.reshape(8),
        offsets.reshape(8, 2),
        object_re,
        object_im,
        probe_re,
        probe_im,
        amplitudes.reshape(8, F, F),
        left,
        right,
    )
    probe_shape = jax.ShapeDtypeStruct((2, F, F), f32)
    return tuple(
        pl.pallas_call(
            write_kernel,
            out_shape=[tile_shape, tile_shape, probe_shape, probe_shape],
            in_specs=[VMEM] * 3,
            out_specs=[VMEM] * 4,
        )(out_re, out_im, flat)
    )


def solution(mesh):
    return jax.shard_map(
        local,
        mesh=mesh,
        in_specs=(
            P("sy", "sx"),
            P("sy", "sx"),
            P(),
            P(),
            P("sy", "sx", None, None, None),
            P("sy", "sx", None, None),
            P("sy", "sx", None),
        ),
        out_specs=(P("sy", "sx"), P("sy", "sx"), P(), P()),
        check_vma=False,
    )
```

```python
import math

import numpy as np

import jax
import jax.numpy as jnp
from jax import lax
from jax.experimental import pallas as pl
from jax.experimental.pallas import tpu as pltpu
from jax.sharding import PartitionSpec as P

MESH = pl.DeviceIdType.MESH
BATCHES = 2
OBJECT_RATE = 0.25
PROBE_GAIN = 4.0
F = 256
H = 128
E = F + 2 * H
ROWS = 16
COLS = 16
SEAM = 8
VMEM = pl.BlockSpec(memory_space=pltpu.VMEM)
SMEM = pl.BlockSpec(memory_space=pltpu.SMEM)
ANY = pl.BlockSpec(memory_space=pl.ANY)
TILE_ROWS = {-1: (H, H), 0: (H, F), 1: (F, H)}
TILE_PLANES = {-1: (1, 1), 0: (1, 2), 1: (2, 1)}
OUTER_ROWS = {-1: (0, H), 0: (H, F), 1: (H + F, H)}
OUTER_PLANES = {-1: (0, 1), 0: (1, 2), 1: (3, 1)}
FRAME_ROWS = {-1: (H + F, H), 0: (H, F), 1: (0, H)}
FRAME_PLANES = {-1: (3, 1), 0: (1, 2), 1: (0, 1)}
INNER_ROWS = {-1: (F, H), 0: (H, F), 1: (H, H)}
INNER_PLANES = {-1: (2, 1), 0: (1, 2), 1: (1, 1)}


def table(frame_size):
    ramp = np.arange(frame_size, dtype=np.int64)
    product = (ramp[:, None] * ramp[None, :]) % frame_size
    angle = np.float32(2.0 * math.pi / frame_size) * product.astype(np.float32)
    scale = np.float32(1.0 / math.sqrt(frame_size))
    return np.cos(angle) * scale, -np.sin(angle) * scale


def dft_operands():
    re, im = table(F)
    left = np.block([[re, -im], [im, re]])
    right = np.block([[re, im], [-im, re]])
    return [jnp.asarray(m, jnp.float32).astype(jnp.bfloat16) for m in (left, right)]


def part(pair):
    return pl.ds(pair[0], pair[1])


def inside(row, col):
    return (row >= 0) & (row < ROWS) & (col >= 0) & (col < COLS)


def greet(peers, meanwhile):
    barrier = pltpu.get_barrier_semaphore()
    count = jnp.int32(0)
    for there, device in peers:

        @pl.when(there)
        def _():
            pl.semaphore_signal(barrier, inc=1, device_id=device, device_id_type=MESH)

        count = count + there.astype(jnp.int32)
    meanwhile()
    pl.semaphore_wait(barrier, count)


class Spot:
    def __init__(self):
        self.row, self.col = lax.axis_index("sy"), lax.axis_index("sx")
        self.half = lax.div(self.col, SEAM)
        self.seat = lax.rem(self.col, SEAM)
        self.seam = (self.col == SEAM - 1) | (self.col == SEAM)
        self.edge = (self.row, SEAM - 1 + self.half)
        self.beyond = (self.row, SEAM - self.half)

    def at(self, dr, dc):
        return (self.row + dr, self.col + dc)

    def has(self, dr, dc):
        return inside(self.row + dr, self.col + dc)

    def far(self, dc):
        return self.col == (SEAM - 1 if dc > 0 else SEAM)

    def peers(self):
        near = [(self.has(dr, dc), self.at(dr, dc)) for dr, dc in ((-1, 0), (1, 0), (0, -1), (0, 1))]
        diagonal = [
            (self.has(dr, dc) & self.far(dc), self.at(dr, dc)) for dr in (-1, 1) for dc in (-1, 1)
        ]
        row, col = self.row, self.col
        relays = [
            (self.seam & (col != c) & (jnp.abs(col - c) != 1), (row, jnp.int32(c))) for c in range(COLS)
        ]
        edges = [(~self.seam & (jnp.abs(col - c) != 1), (row, jnp.int32(c))) for c in (SEAM - 1, SEAM)]
        return near + diagonal + relays[: SEAM - 1] + relays[SEAM + 1 :] + [
            (self.seam & (there), device) for there, device in relays[SEAM - 1 : SEAM + 1]
        ] + edges


def remote(src, dst, sems, at, device):
    return pltpu.make_async_remote_copy(
        src_ref=src,
        dst_ref=dst,
        send_sem=sems[0].at[at],
        recv_sem=sems[1].at[at],
        device_id=device,
        device_id_type=MESH,
    )


class Transfers:
    def __init__(self, entries):
        self.entries = entries

    def start(self):
        for sent, received, build in self.entries:

            @pl.when(sent)
            def _():
                build().start()

    def wait_recv(self):
        for sent, received, build in self.entries:

            @pl.when(received)
            def _():
                build().wait_recv()

    def wait_send(self):
        for sent, received, build in self.entries:

            @pl.when(sent)
            def _():
                build().wait_send()


SIDES = (-1, 1)


def clear_edges(row, col, frame):
    @pl.when(row == 0)
    def _():
        frame[:, :, 0:H, :] = jnp.zeros((2, 4, H, H), jnp.float32)

    @pl.when(row == ROWS - 1)
    def _():
        frame[:, :, H + F : E, :] = jnp.zeros((2, 4, H, H), jnp.float32)

    @pl.when(col == 0)
    def _():
        frame[:, 0] = jnp.zeros((2, E, H), jnp.float32)

    @pl.when(col == COLS - 1)
    def _():
        frame[:, 3] = jnp.zeros((2, E, H), jnp.float32)


FOUR = [(k, n) for k in range(2) for n in range(2)]
SLICE = F // SEAM


class Relay:
    def __init__(self, spot, source, target, held, first, second):
        self.spot, self.source, self.target, self.held = spot, source, target, held
        self.first, self.second = first, second

    def out(self, q):
        spot = self.spot
        device = (spot.row, spot.half * SEAM + q)
        return remote(self.source(q * SLICE), self.held, self.first, q, device)

    def arrive(self):
        return pltpu.make_async_remote_copy(
            src_ref=self.held, dst_ref=self.held, send_sem=self.first[0].at[0],
            recv_sem=self.first[1].at[self.spot.seat], device_id=self.spot.edge, device_id_type=MESH,
        )

    def on(self, q, src):
        return remote(src, self.target(pl.multiple_of(q * SLICE, SLICE)), self.second, q, self.spot.beyond)

    def start(self):
        spot = self.spot
        for q in range(SEAM):

            @pl.when(spot.seam & (spot.seat != q))
            def _():
                self.out(q).start()

        for half, q in ((0, SEAM - 1), (1, 0)):

            @pl.when(spot.seam & (spot.half == half))
            def _():
                self.on(q, self.source(q * SLICE)).start()

    def turn(self):
        @pl.when(~self.spot.seam)
        def _():
            self.arrive().wait_recv()
            self.on(self.spot.seat, self.held).start()

    def wait_recv(self):
        @pl.when(self.spot.seam)
        def _():
            for q in range(SEAM):
                self.on(q, self.held).wait_recv()

    def wait_send(self):
        spot = self.spot

        @pl.when(~spot.seam)
        def _():
            self.on(spot.seat, self.held).wait_send()

        for q in range(SEAM):

            @pl.when(spot.seam & (spot.seat != q))
            def _():
                self.out(q).wait_send()

        for half, q in ((0, SEAM - 1), (1, 0)):

            @pl.when(spot.seam & (spot.half == half))
            def _():
                self.on(q, self.held).wait_send()


class Halo:
    def __init__(self, spot, frame, held, upright, level, corner, seam, first, second):
        self.spot, self.frame = spot, frame

        def strip(ch, dr, planes, rows_from, to_rows, to_planes, sems, k, device):
            c = pl.ds(ch, 1)
            return lambda: remote(
                frame.at[c, part(planes), part(rows_from)], frame.at[c, part(to_planes), part(to_rows)], sems, (ch, k), device
            )

        def both(make):
            return [Transfers(make(ch)) for ch in range(2)]

        self.vertical = both(lambda ch: [
            (
                spot.has(dr, 0),
                spot.has(-dr, 0),
                strip(ch, dr, (1, 2), TILE_ROWS[dr], FRAME_ROWS[dr], (1, 2), upright, k, spot.at(dr, 0)),
            )
            for k, dr in enumerate(SIDES)
        ])
        self.across = both(lambda ch: [
            (
                spot.has(dr, dc) & spot.far(dc),
                spot.has(-dr, -dc) & spot.far(-dc),
                strip(ch, dr, TILE_PLANES[dc], TILE_ROWS[dr], FRAME_ROWS[dr], FRAME_PLANES[dc], seam, 2 * k + n, spot.at(dr, dc)),
            )
            for k, dr in enumerate(SIDES)
            for n, dc in enumerate(SIDES)
        ])
        self.middle = both(lambda ch: [
            (
                spot.has(0, dc) & ~spot.far(dc),
                spot.has(0, -dc) & ~spot.far(-dc),
                strip(ch, 0, TILE_PLANES[dc], (H, F), (H, F), FRAME_PLANES[dc], level, n, spot.at(0, dc)),
            )
            for n, dc in enumerate(SIDES)
        ])
        self.corners = both(lambda ch: [
            (
                spot.has(side, 0) & spot.has(0, dc) & ~spot.far(dc),
                spot.has(side, 0) & spot.has(0, -dc) & ~spot.far(-dc),
                strip(ch, 0, TILE_PLANES[dc], OUTER_ROWS[side], OUTER_ROWS[side], FRAME_PLANES[dc], corner, 2 * k + n, spot.at(0, dc)),
            )
            for k, side in enumerate(SIDES)
            for n, dc in enumerate(SIDES)
        ])
        half = spot.half
        self.relay = Relay(
            spot,
            lambda row: frame.at[:, pl.ds(2 - half, 1), pl.ds(H + row, SLICE)],
            lambda row: frame.at[:, pl.ds(3 * half, 1), pl.ds(H + row, SLICE)],
            held, first, second,
        )

    def begin(self, ch):
        self.vertical[ch].start()
        self.across[ch].start()

    def aside(self):
        self.relay.start()
        self.middle[0].start()
        self.middle[1].start()
        self.relay.turn()

    def end(self):
        for ch in range(2):
            self.vertical[ch].wait_recv()
            self.corners[ch].start()
        for ch in range(2):
            self.middle[ch].wait_recv()
        self.relay.wait_recv()
        for ch in range(2):
            for transfers in (self.across[ch], self.corners[ch]):
                transfers.wait_recv()
        for ch in range(2):
            for transfers in (self.vertical[ch], self.middle[ch], self.across[ch], self.corners[ch]):
                transfers.wait_send()
        self.relay.wait_send()


def pairs(sems):
    return [(sems[i], sems[i + 1]) for i in range(0, len(sems), 2)]


class Fold:
    def __init__(self, spot, accum, cbuf, mbuf, vbuf, fbuf, stack, held, upright, level, corner, seam, first, second):
        self.spot, self.accum, self.stack = spot, accum, stack
        self.cbuf, self.mbuf, self.vbuf, self.fbuf = cbuf, mbuf, vbuf, fbuf

        def strip(ch, planes, rows, buf, sems, k, device):
            return lambda: remote(accum.at[ch, part(planes), part(rows)], buf.at[ch, k], sems, (ch, k), device)

        def both(make):
            return [Transfers(make(ch)) for ch in range(2)]

        self.corners = both(lambda ch: [
            (
                spot.has(side, 0) & spot.has(0, dc) & ~spot.far(dc),
                spot.has(side, 0) & spot.has(0, -dc) & ~spot.far(-dc),
                strip(ch, OUTER_PLANES[dc], OUTER_ROWS[side], cbuf, corner, 2 * k + n, spot.at(0, dc)),
            )
            for k, side in enumerate(SIDES)
            for n, dc in enumerate(SIDES)
        ])
        self.across = both(lambda ch: [
            (
                spot.has(dr, dc) & spot.far(dc),
                spot.has(-dr, -dc) & spot.far(-dc),
                strip(ch, OUTER_PLANES[dc], OUTER_ROWS[dr], fbuf, seam, 2 * k + n, spot.at(dr, dc)),
            )
            for k, dr in enumerate(SIDES)
            for n, dc in enumerate(SIDES)
        ])
        self.middle = both(lambda ch: [
            (
                spot.has(0, dc) & ~spot.far(dc),
                spot.has(0, -dc) & ~spot.far(-dc),
                strip(ch, OUTER_PLANES[dc], (H, F), mbuf, level, n, spot.at(0, dc)),
            )
            for n, dc in enumerate(SIDES)
        ])
        self.vertical = both(lambda ch: [
            (
                spot.has(dr, 0),
                spot.has(-dr, 0),
                lambda k=k, dr=dr: remote(stack.at[ch, k], vbuf.at[ch, k], upright, (ch, k), spot.at(dr, 0)),
            )
            for k, dr in enumerate(SIDES)
        ])
        half = spot.half
        self.relay = Relay(
            spot,
            lambda row: accum.at[:, pl.ds(3 - 3 * half, 1), pl.ds(H + row, SLICE)],
            lambda row: mbuf.at[:, 1 - half, :, pl.ds(row, SLICE)],
            held, first, second,
        )

    def begin(self):
        self.corners[0].start()
        self.corners[1].start()

    def aside(self):
        self.relay.start()
        self.middle[0].start()
        self.middle[1].start()

    def turn(self, ch):
        stack, cbuf = self.stack, self.cbuf
        for k, side in enumerate(SIDES):
            stack[ch, k] = self.accum[ch, 1:3, part(OUTER_ROWS[side])]
        self.corners[ch].wait_recv()
        for (_, received, _), (k, n) in zip(self.corners[ch].entries, FOUR):

            @pl.when(received)
            def _():
                plane = INNER_PLANES[SIDES[n]][0] - 1
                stack[ch, k, plane] = stack[ch, k, plane] + cbuf[ch, 2 * k + n, 0]

        self.vertical[ch].start()
        self.across[ch].start()

    def end(self, ch, add):
        spot = self.spot
        self.middle[ch].wait_recv()
        if ch == 0:
            self.relay.wait_recv()
        for n, dc in enumerate(SIDES):

            @pl.when(spot.has(0, -dc))
            def _():
                add(self.mbuf.at[ch, n], (H, F), INNER_PLANES[dc])

        self.vertical[ch].wait_recv()
        for k, dr in enumerate(SIDES):

            @pl.when(spot.has(-dr, 0))
            def _():
                add(self.vbuf.at[ch, k], INNER_ROWS[dr], (1, 2))

        self.across[ch].wait_recv()
        for (_, received, _), (k, n) in zip(self.across[ch].entries, FOUR):

            @pl.when(received)
            def _():
                add(self.fbuf.at[ch, 2 * k + n], INNER_ROWS[SIDES[k]], INNER_PLANES[SIDES[n]])

    def close(self):
        for ch in range(2):
            for transfers in (self.corners[ch], self.across[ch], self.middle[ch], self.vertical[ch]):
                transfers.wait_send()
        self.relay.wait_send()


def renew(spot, fold, halo, accum, frame, place_channel):
    for ch in range(2):
        place_channel(ch)
        fold.corners[ch].start()
    fold.aside()
    fold.turn(0)
    fold.turn(1)
    fold.relay.turn()
    frame[:, 1:3, H : H + F] = frame[:, 1:3, H : H + F] + accum[:, 1:3, H : H + F]
    for ch in range(2):

        def add(buf, rows, planes):
            where = (ch, part(planes), part(rows))
            frame[where] = frame[where] + buf[...]

        fold.end(ch, add)
        halo.begin(ch)
    halo.aside()
    halo.end()
    fold.close()


def held_buffer():
    return pltpu.VMEM((2, 1, SLICE, H), jnp.float32)


def fold_buffers():
    f32 = jnp.float32
    return [
        pltpu.VMEM((2, 4, 1, H, H), f32),
        pltpu.VMEM((2, 2, 1, F, H), f32),
        pltpu.VMEM((2, 2, 2, H, H), f32),
        pltpu.VMEM((2, 4, 1, H, H), f32),
        pltpu.VMEM((2, 2, 2, H, H), f32),
        held_buffer(),
    ]


def exchange_sems():
    dma = pltpu.SemaphoreType.DMA
    shapes = ((2, 2), (2, 2), (2, 4), (2, 4), (SEAM,), (SEAM,))
    return [dma(shape) for shape in shapes for _ in range(2)]


CHUNK1 = 64
CHUNK2 = 16
COLORS = (("x", "y"), ("y", "x"))


def torus():
    sy, sx = lax.axis_index("sy"), lax.axis_index("sx")
    here = {
        "y": lax.div(sy, 4),
        "x": lax.div(lax.rem(sx, 8), 2),
        "z": lax.div(sx, 8) * 4 + lax.rem(sy, 4),
        "core": lax.rem(sx, 2),
    }
    size = {"x": 4, "y": 4, "z": 8, "core": 2}

    def place(axis, step):
        there = dict(here)
        there[axis] = lax.rem(here[axis] + step, size[axis])
        device = (
            there["y"] * 4 + lax.rem(there["z"], 4),
            lax.div(there["z"], 4) * 8 + there["x"] * 2 + there["core"],
        )
        return there[axis], device

    return here, place


def finish_all(fold, place_channel, accum, old, g, probe_re, probe_im, out_re, out_im, out, *rest):
    r0, w0, r1, w1, r2, w2, r3, w4, s0, q0, s1, q1, s2, q2, s3, q3, s4, q4, s5, q5, s6, q6 = rest
    here, place = torus()
    rate = PROBE_GAIN / (8 * math.sqrt(ROWS * COLS))
    core = here["core"]
    other, partner = place("core", 1)
    mine = pl.ds(pl.multiple_of(core * 512, 512), 512)
    theirs = pl.ds(pl.multiple_of(other * 512, 512), 512)

    def send(src, dst, ss, rs, device):
        copy = pltpu.make_async_remote_copy(
            src_ref=src, dst_ref=dst, send_sem=ss, recv_sem=rs, device_id=device, device_id_type=MESH
        )
        copy.start()
        return copy

    def rows(start, count):
        return pl.ds(pl.multiple_of(start, count), count)

    def wait(copies):
        for copy in copies:
            copy.wait()

    across_cores = send(g.at[theirs], r0, s0, q0, partner)
    place_channel(0)
    place_channel(1)
    across_cores.wait()
    w0[...] = g[mine] + r0[...]

    copies = []
    for c, (first, second) in enumerate(COLORS):
        copies.append([])
        for step in (1, 2, 3):
            index, device = place(first, step)
            source = w0.at[rows(c * 256 + index * CHUNK1, CHUNK1)]
            copies[c].append(send(source, r1.at[c, step - 1], s1.at[c, step - 1], q1.at[c, step - 1], device))
    fold.begin()
    for c, (first, second) in enumerate(COLORS):
        wait(copies[c])
        own = w0[rows(c * 256 + here[first] * CHUNK1, CHUNK1)]
        w1[c] = (own + r1[c, 0]) + (r1[c, 1] + r1[c, 2])
        copies[c] = []
        for step in (1, 2, 3):
            index, device = place(second, step)
            source = w1.at[c, rows(index * CHUNK2, CHUNK2)]
            copies[c].append(send(source, r2.at[c, step - 1], s2.at[c, step - 1], q2.at[c, step - 1], device))
    fold.turn(0)
    for c, (first, second) in enumerate(COLORS):
        wait(copies[c])
        own = w1[c, rows(here[second] * CHUNK2, CHUNK2)]
        w2[c] = (own + r2[c, 0]) + (r2[c, 1] + r2[c, 2])
        copies[c] = []
        for step in range(1, 8):
            device = place("z", step)[1]
            copies[c].append(send(w2.at[c], r3.at[c, here["z"]], s3.at[c, step - 1], q3.at[c, step - 1], device))
        r3[c, here["z"]] = w2[c]
    fold.turn(1)
    fold.aside()
    fold.relay.turn()
    outs = (out_re, out_im)
    for channel, tile in enumerate(outs):
        for n in range(2):
            tile[:, n * H : (n + 1) * H] = old[channel, 1 + n, H : H + F] + accum[channel, 1 + n, H : H + F]
    for c, (first, second) in enumerate(COLORS):
        wait(copies[c])
        total = ((r3[c, 0] + r3[c, 1]) + (r3[c, 2] + r3[c, 3])) + ((r3[c, 4] + r3[c, 5]) + (r3[c, 6] + r3[c, 7]))
        start = c * 256 + here[first] * CHUNK1 + here[second] * CHUNK2
        own = rows(lax.rem(start, F), CHUNK2)
        mode = lax.div(start, F)
        base = jnp.where(core == 0, probe_re[mode, own], probe_im[mode, own])
        spot = rows(here[second] * CHUNK2, CHUNK2)
        w4[c, spot] = base + rate * total
        copies[c] = []
        for step in (1, 2, 3):
            device = place(second, step)[1]
            copies[c].append(send(w4.at[c, spot], w4.at[c, spot], s4.at[c, step - 1], q4.at[c, step - 1], device))
    last = []
    for c, (first, second) in enumerate(COLORS):
        wait(copies[c])
        spot = out.at[rows(core * 512 + c * 256 + here[first] * CHUNK1, CHUNK1)]
        copies[c] = []
        for step in (1, 2, 3):
            device = place(first, step)[1]
            copies[c].append(send(w4.at[c], spot, s5.at[c, step - 1], q5.at[c, step - 1], device))
        out[rows(core * 512 + c * 256 + here[first] * CHUNK1, CHUNK1)] = w4[c]
        last.append(send(w4.at[c], spot, s6.at[c, 0], q6.at[c, 0], partner))
    for ch, tile in enumerate(outs):

        def add(buf, where_rows, planes):
            for n in range(planes[1]):
                where = (pl.ds(where_rows[0] - H, where_rows[1]), pl.ds((planes[0] - 1 + n) * H, H))
                tile[where] = tile[where] + buf[n]

        fold.end(ch, add)
    for c, (first, second) in enumerate(COLORS):
        for step in (1, 2, 3):
            copies[c][step - 1].wait()
            source = place(first, 4 - step)[0]
            spot = out.at[rows(core * 512 + c * 256 + source * CHUNK1, CHUNK1)]
            last.append(send(spot, spot, s6.at[c, step], q6.at[c, step], partner))
    fold.close()
    wait(last)


def write_kernel(a, b, flat, out_a, out_b, out_c, out_d, held_a, held_b, held_flat, load_sem, store_sem):
    parts = [(a, held_a, out_a), (b, held_b, out_b)]
    for k, out in enumerate((out_c, out_d)):
        for m in range(2):
            rows = pl.ds((2 * k + m) * F, F)
            parts.append((flat.at[rows], held_flat.at[rows], out.at[m]))
    loads = [pltpu.make_async_copy(src, held, load_sem.at[i]) for i, (src, held, _) in enumerate(parts)]
    stores = [pltpu.make_async_copy(held, out, store_sem.at[i]) for i, (_, held, out) in enumerate(parts)]
    for load in loads:
        load.start()
    for load, store in zip(loads, stores):
        load.wait()
        store.start()
    for store in stores:
        store.wait()


def place_terms(ch, batch, order, offsets, accum, padded):
    starts = []
    for j in range(4):
        starts.append(F - (offsets[0, 0, 0, order[0, 0, batch * 4 + j]] + H))
    for n in range(4):
        for row in range(0, E, H):
            parts = [padded[j, ch, n, pl.ds(starts[j] + row, H), :] for j in range(4)]
            accum[ch, n, row : row + H, :] = (parts[0] + parts[1]) + (parts[2] + parts[3])


def work(batch, order, offsets, frame, probe_re, probe_im, amps, amp_ready, left, right, accum, grad, scale, padded, patch, fields, halves):
    back_left, back_right = right, left
    size = 4
    for j in range(size):
        p = order[0, 0, batch * size + j]
        top = offsets[0, 0, 0, p] + H
        shift = offsets[0, 0, 1, p] + H
        for ch in range(2):
            rows = jnp.concatenate([frame[ch, n, pl.ds(top, F), :] for n in range(4)], axis=1)
            patch[j, ch] = pltpu.roll(rows, lax.rem(E - shift, E), 1)[:, :F]
        re, im = patch[j, 0], patch[j, 1]
        for m in range(2):
            at = pl.ds((2 * j + m) * F, F)
            fields[0:F, at] = (probe_re[m] * re - probe_im[m] * im).astype(jnp.bfloat16)
            fields[F : 2 * F, at] = (probe_re[m] * im + probe_im[m] * re).astype(jnp.bfloat16)
    for n in range(2 * size):
        half = jnp.dot(left[...], fields[0 : 2 * F, n * F : (n + 1) * F], preferred_element_type=jnp.float32)
        halves[n * F : (n + 1) * F, 0:F] = half[0:F].astype(jnp.bfloat16)
        halves[n * F : (n + 1) * F, F : 2 * F] = half[F:].astype(jnp.bfloat16)
    for j in range(size):
        far = jnp.dot(halves[2 * j * F : 2 * (j + 1) * F, :], right[...], preferred_element_type=jnp.float32)
        squares = far * far
        intensity = (squares[0:F, 0:F] + squares[0:F, F:]) + (squares[F:, 0:F] + squares[F:, F:])
        if j == 0:
            amp_ready()
        ratio = amps[order[0, 0, batch * size + j]] * lax.rsqrt(jnp.maximum(intensity, 1.0))
        for m in range(2):
            at = (2 * j + m) * F
            fields[2 * F : 3 * F, at : at + F] = (far[m * F : (m + 1) * F, 0:F] * ratio).astype(jnp.bfloat16)
            fields[3 * F : 4 * F, at : at + F] = (far[m * F : (m + 1) * F, F:] * ratio).astype(jnp.bfloat16)
    for n in range(2 * size):
        half = jnp.dot(back_left[...], fields[2 * F :, n * F : (n + 1) * F], preferred_element_type=jnp.float32)
        halves[n * F : (n + 1) * F, 0:F] = half[0:F].astype(jnp.bfloat16)
        halves[n * F : (n + 1) * F, F : 2 * F] = half[F:].astype(jnp.bfloat16)
    for j in range(size):
        p = order[0, 0, batch * size + j]
        top = offsets[0, 0, 0, p] + H
        shift = offsets[0, 0, 1, p] + H
        back = jnp.dot(halves[2 * j * F : 2 * (j + 1) * F, :], back_right[...], preferred_element_type=jnp.float32)
        re, im = patch[j, 0], patch[j, 1]
        terms = [None, None]
        for m in range(2):
            at = (2 * j + m) * F
            d_re = back[m * F : (m + 1) * F, 0:F] - fields[0:F, at : at + F].astype(jnp.float32)
            d_im = back[m * F : (m + 1) * F, F:] - fields[F : 2 * F, at : at + F].astype(jnp.float32)
            o_re = probe_re[m] * d_re + probe_im[m] * d_im
            o_im = probe_re[m] * d_im - probe_im[m] * d_re
            g_re = re * d_re + im * d_im
            g_im = re * d_im - im * d_re
            if m == 0:
                terms = [o_re, o_im]
            else:
                terms = [terms[0] + o_re, terms[1] + o_im]
            for ch, g in enumerate((g_re, g_im)):
                own = pl.ds((2 * ch + m) * F, F)
                if j == 0 and batch == 0:
                    grad[own] = g
                else:
                    grad[own] = grad[own] + g
        for ch in range(2):
            wide = jnp.concatenate([terms[ch] * scale[0:1, 0:1], jnp.zeros((F, F), jnp.float32)], axis=1)
            wide = pltpu.roll(wide, shift, 1)
            for n in range(4):
                padded[j, ch, n, F : 2 * F, :] = wide[:, n * H : (n + 1) * H]


def whole_kernel(order, offsets, re_ref, im_ref, probe_re_in, probe_im_in, amps_in, left_in, right_in, out_re, out_im, out, *scratch):
    frame, accum, probe_re, probe_im, amps, left, right, grad, scale, padded, patch, fields, halves, load_sem = scratch[:14]
    buffers, sems, rest = scratch[14:28], pairs(scratch[28:76]), scratch[76:]
    spot = Spot()
    loads = [
        pltpu.make_async_copy(source, target, load_sem.at[i])
        for i, (source, target) in enumerate(
            [(probe_re_in, probe_re), (probe_im_in, probe_im), (left_in, left), (right_in, right), (amps_in, amps)]
        )
    ]
    for load in loads:
        load.start()

    def meanwhile():
        for channel, source in enumerate((re_ref, im_ref)):
            for n in range(2):
                frame[channel, 1 + n, H : H + F] = source[:, n * H : (n + 1) * H]
        clear_edges(spot.row, spot.col, frame)

    here, place = torus()
    yes = spot.row >= 0
    size = {"core": 2, "x": 4, "y": 4, "z": 8}
    greet(
        spot.peers()
        + [(yes, place(axis, step)[1]) for axis in size for step in range(1, size[axis])],
        meanwhile,
    )
    halo = Halo(spot, frame, buffers[12], *sems[0:6])
    halo.begin(0)
    halo.begin(1)
    halo.aside()
    blank = jnp.zeros((F, H), jnp.float32)
    for j in range(4):
        for ch in range(2):
            for n in range(4):
                padded[j, ch, n, 0:F] = blank
                padded[j, ch, n, 2 * F : 3 * F] = blank
    for load in loads[:4]:
        load.wait()
    power = jnp.max(
        probe_re[0] * probe_re[0]
        + probe_im[0] * probe_im[0]
        + (probe_re[1] * probe_re[1] + probe_im[1] * probe_im[1]),
        keepdims=True,
    )
    scale[...] = jnp.broadcast_to(OBJECT_RATE / power, (8, H))
    halo.end()
    common = (left, right, accum, grad, scale, padded, patch, fields, halves)
    work(0, order, offsets, frame, probe_re, probe_im, amps, loads[4].wait, *common)
    fold = Fold(spot, accum, *buffers[0:6], *sems[6:12])
    halo = Halo(spot, frame, buffers[13], *sems[12:18])
    renew(spot, fold, halo, accum, frame, lambda ch: place_terms(ch, 0, order, offsets, accum, padded))
    work(1, order, offsets, frame, probe_re, probe_im, amps, lambda: None, *common)
    fold = Fold(spot, accum, *buffers[6:12], *sems[18:24])
    finish_all(fold, lambda ch: place_terms(ch, 1, order, offsets, accum, padded), accum, frame, grad, probe_re, probe_im, out_re, out_im, out, *rest)


def local(object_re, object_im, probe_re, probe_im, amplitudes, offsets, visit_order):
    f32, bf16 = jnp.float32, jnp.bfloat16
    left, right = dft_operands()
    dma = pltpu.SemaphoreType.DMA
    tile_shape = jax.ShapeDtypeStruct((F, F), f32)
    out_re, out_im, flat = pl.pallas_call(
        whole_kernel,
        out_shape=[tile_shape, tile_shape, jax.ShapeDtypeStruct((4 * F, F), f32)],
        in_specs=[SMEM, SMEM, VMEM, VMEM, ANY, ANY, ANY, ANY, ANY],
        out_specs=[VMEM] * 3,
        scratch_shapes=[
            pltpu.VMEM((2, 4, E, H), f32),
            pltpu.VMEM((2, 4, E, H), f32),
            pltpu.VMEM((2, F, F), f32),
            pltpu.VMEM((2, F, F), f32),
            pltpu.VMEM((8, F, F), f32),
            pltpu.VMEM((2 * F, 2 * F), bf16),
            pltpu.VMEM((2 * F, 2 * F), bf16),
            pltpu.VMEM((4 * F, F), f32),
            pltpu.VMEM((8, H), f32),
            pltpu.VMEM((4, 2, 4, 3 * F, H), f32),
            pltpu.VMEM((4, 2, F, F), f32),
            pltpu.VMEM((4 * F, 8 * F), bf16),
            pltpu.VMEM((8 * F, 2 * F), bf16),
            dma((5,)),
        ]
        + fold_buffers()
        + fold_buffers()
        + [held_buffer(), held_buffer()]
        + exchange_sems() * 4
        + [
            pltpu.VMEM((512, F), f32),
            pltpu.VMEM((512, F), f32),
            pltpu.VMEM((2, 3, CHUNK1, F), f32),
            pltpu.VMEM((2, CHUNK1, F), f32),
            pltpu.VMEM((2, 3, CHUNK2, F), f32),
            pltpu.VMEM((2, CHUNK2, F), f32),
            pltpu.VMEM((2, 8, CHUNK2, F), f32),
            pltpu.VMEM((2, CHUNK1, F), f32),
            dma, dma,
            dma((2, 3)), dma((2, 3)),
            dma((2, 3)), dma((2, 3)),
            dma((2, 7)), dma((2, 7)),
            dma((2, 3)), dma((2, 3)),
            dma((2, 3)), dma((2, 3)),
            dma((2, 4)), dma((2, 4)),
        ],
        compiler_params=pltpu.CompilerParams(
            collective_id=0, has_side_effects=True, vmem_limit_bytes=62 * 1024 * 1024
        ),
    )(
        visit_order,
        jnp.swapaxes(offsets, 2, 3),
        object_re,
        object_im,
        probe_re,
        probe_im,
        amplitudes.reshape(8, F, F),
        left,
        right,
    )
    probe_shape = jax.ShapeDtypeStruct((2, F, F), f32)
    return tuple(
        pl.pallas_call(
            write_kernel,
            out_shape=[tile_shape, tile_shape, probe_shape, probe_shape],
            in_specs=[ANY] * 3,
            out_specs=[ANY] * 4,
            scratch_shapes=[
                pltpu.VMEM((F, F), f32),
                pltpu.VMEM((F, F), f32),
                pltpu.VMEM((4 * F, F), f32),
                dma((6,)),
                dma((6,)),
            ],
        )(out_re, out_im, flat)
    )


def solution(mesh):
    return jax.shard_map(
        local,
        mesh=mesh,
        in_specs=(
            P("sy", "sx"),
            P("sy", "sx"),
            P(),
            P(),
            P("sy", "sx", None, None, None),
            P("sy", "sx", None, None),
            P("sy", "sx", None),
        ),
        out_specs=(P("sy", "sx"), P("sy", "sx"), P(), P()),
        check_vma=False,
    )
```

```python
import math

import numpy as np

import jax
import jax.numpy as jnp
from jax import lax
from jax.experimental import pallas as pl
from jax.experimental.pallas import tpu as pltpu
from jax.sharding import PartitionSpec as P

MESH = pl.DeviceIdType.MESH
BATCHES = 2
OBJECT_RATE = 0.25
PROBE_GAIN = 4.0
F = 256
H = 128
E = F + 2 * H
ROWS = 16
COLS = 16
SEAM = 8
VMEM = pl.BlockSpec(memory_space=pltpu.VMEM)
SMEM = pl.BlockSpec(memory_space=pltpu.SMEM)
ANY = pl.BlockSpec(memory_space=pl.ANY)
TILE_ROWS = {-1: (H, H), 0: (H, F), 1: (F, H)}
TILE_PLANES = {-1: (1, 1), 0: (1, 2), 1: (2, 1)}
OUTER_ROWS = {-1: (0, H), 0: (H, F), 1: (H + F, H)}
OUTER_PLANES = {-1: (0, 1), 0: (1, 2), 1: (3, 1)}
FRAME_ROWS = {-1: (H + F, H), 0: (H, F), 1: (0, H)}
FRAME_PLANES = {-1: (3, 1), 0: (1, 2), 1: (0, 1)}
INNER_ROWS = {-1: (F, H), 0: (H, F), 1: (H, H)}
INNER_PLANES = {-1: (2, 1), 0: (1, 2), 1: (1, 1)}


def table(frame_size):
    ramp = np.arange(frame_size, dtype=np.int64)
    product = (ramp[:, None] * ramp[None, :]) % frame_size
    angle = np.float32(2.0 * math.pi / frame_size) * product.astype(np.float32)
    scale = np.float32(1.0 / math.sqrt(frame_size))
    return np.cos(angle) * scale, -np.sin(angle) * scale


def dft_operands():
    re, im = table(F)
    left = np.block([[re, -im], [im, re]])
    right = np.block([[re, im], [-im, re]])
    return [jnp.asarray(m, jnp.float32).astype(jnp.bfloat16) for m in (left, right)]


def part(pair):
    return pl.ds(pair[0], pair[1])


def inside(row, col):
    return (row >= 0) & (row < ROWS) & (col >= 0) & (col < COLS)


def greet(peers, meanwhile):
    barrier = pltpu.get_barrier_semaphore()
    count = jnp.int32(0)
    for there, device in peers:

        @pl.when(there)
        def _():
            pl.semaphore_signal(barrier, inc=1, device_id=device, device_id_type=MESH)

        count = count + there.astype(jnp.int32)
    meanwhile()
    pl.semaphore_wait(barrier, count)


class Spot:
    def __init__(self):
        self.row, self.col = lax.axis_index("sy"), lax.axis_index("sx")
        self.half = lax.div(self.col, SEAM)
        self.seat = lax.rem(self.col, SEAM)
        self.seam = (self.col == SEAM - 1) | (self.col == SEAM)
        self.edge = (self.row, SEAM - 1 + self.half)
        self.beyond = (self.row, SEAM - self.half)

    def at(self, dr, dc):
        return (self.row + dr, self.col + dc)

    def has(self, dr, dc):
        return inside(self.row + dr, self.col + dc)

    def far(self, dc):
        return self.col == (SEAM - 1 if dc > 0 else SEAM)

    def peers(self):
        near = [(self.has(dr, dc), self.at(dr, dc)) for dr, dc in ((-1, 0), (1, 0), (0, -1), (0, 1))]
        diagonal = [
            (self.has(dr, dc) & self.far(dc), self.at(dr, dc)) for dr in (-1, 1) for dc in (-1, 1)
        ]
        row, col = self.row, self.col
        relays = [
            (self.seam & (col != c) & (jnp.abs(col - c) != 1), (row, jnp.int32(c))) for c in range(COLS)
        ]
        edges = [(~self.seam & (jnp.abs(col - c) != 1), (row, jnp.int32(c))) for c in (SEAM - 1, SEAM)]
        slants = [
            (self.has(dr, 0) & (self.half == 1 - half) & there, (row + dr, device[1]))
            for half in (0, 1)
            for dr in (-1, 1)
            for there, device in (
                [(self.col == SEAM - half, (row, jnp.int32(c))) for c in range(half * SEAM, half * SEAM + SEAM) if c not in (SEAM - 1, SEAM)]
                + [(~self.seam, (row, jnp.int32(SEAM - 1 + half)))]
            )
        ]
        return near + diagonal + slants + relays[: SEAM - 1] + relays[SEAM + 1 :] + [
            (self.seam & (there), device) for there, device in relays[SEAM - 1 : SEAM + 1]
        ] + edges


def remote(src, dst, sems, at, device):
    return pltpu.make_async_remote_copy(
        src_ref=src,
        dst_ref=dst,
        send_sem=sems[0].at[at],
        recv_sem=sems[1].at[at],
        device_id=device,
        device_id_type=MESH,
    )


class Transfers:
    def __init__(self, entries):
        self.entries = entries

    def start(self):
        for sent, received, build in self.entries:

            @pl.when(sent)
            def _():
                build().start()

    def wait_recv(self):
        for sent, received, build in self.entries:

            @pl.when(received)
            def _():
                build().wait_recv()

    def wait_send(self):
        for sent, received, build in self.entries:

            @pl.when(sent)
            def _():
                build().wait_send()


SIDES = (-1, 1)


def clear_edges(row, col, frame):
    @pl.when(row == 0)
    def _():
        frame[:, :, 0:H, :] = jnp.zeros((2, 4, H, H), jnp.float32)

    @pl.when(row == ROWS - 1)
    def _():
        frame[:, :, H + F : E, :] = jnp.zeros((2, 4, H, H), jnp.float32)

    @pl.when(col == 0)
    def _():
        frame[:, 0] = jnp.zeros((2, E, H), jnp.float32)

    @pl.when(col == COLS - 1)
    def _():
        frame[:, 3] = jnp.zeros((2, E, H), jnp.float32)


FOUR = [(k, n) for k in range(2) for n in range(2)]
STRIPS = ((-1, H // SEAM), (1, H // SEAM), (0, F // SEAM))


class Relay:
    def __init__(self, spot, dr, count, source, target, held, first, second):
        self.spot, self.source, self.target, self.held = spot, source, target, held
        self.first, self.second, self.count = first, second, count
        self.sends, self.gets = spot.has(dr, 0), spot.seam & spot.has(-dr, 0)
        self.goal = (spot.row + dr, spot.beyond[1])

    def out(self, q):
        spot = self.spot
        device = (spot.row, spot.half * SEAM + q)
        return remote(self.source(q * self.count), self.held, self.first, q, device)

    def arrive(self):
        return pltpu.make_async_remote_copy(
            src_ref=self.held, dst_ref=self.held, send_sem=self.first[0].at[0],
            recv_sem=self.first[1].at[self.spot.seat], device_id=self.spot.edge, device_id_type=MESH,
        )

    def on(self, q, src):
        return remote(src, self.target(pl.multiple_of(q * self.count, self.count)), self.second, q, self.goal)

    def start(self):
        spot = self.spot
        for q in range(SEAM):

            @pl.when(self.sends & spot.seam & (spot.seat != q))
            def _():
                self.out(q).start()

        for half, q in ((0, SEAM - 1), (1, 0)):

            @pl.when(self.sends & spot.seam & (spot.half == half))
            def _():
                self.on(q, self.source(q * self.count)).start()

    def turn(self):
        @pl.when(self.sends & ~self.spot.seam)
        def _():
            self.arrive().wait_recv()
            self.on(self.spot.seat, self.held).start()

    def wait_recv(self):
        @pl.when(self.gets)
        def _():
            for q in range(SEAM):
                self.on(q, self.held).wait_recv()

    def wait_send(self):
        spot = self.spot

        @pl.when(self.sends & ~spot.seam)
        def _():
            self.on(spot.seat, self.held).wait_send()

        for q in range(SEAM):

            @pl.when(self.sends & spot.seam & (spot.seat != q))
            def _():
                self.out(q).wait_send()

        for half, q in ((0, SEAM - 1), (1, 0)):

            @pl.when(self.sends & spot.seam & (spot.half == half))
            def _():
                self.on(q, self.held).wait_send()


class Halo:
    def __init__(self, spot, frame, held, upright, level, corner, *relay_sems):
        self.spot, self.frame = spot, frame

        def strip(ch, dr, planes, rows_from, to_rows, to_planes, sems, k, device):
            c = pl.ds(ch, 1)
            return lambda: remote(
                frame.at[c, part(planes), part(rows_from)], frame.at[c, part(to_planes), part(to_rows)], sems, (ch, k), device
            )

        def both(make):
            return [Transfers(make(ch)) for ch in range(2)]

        self.vertical = both(lambda ch: [
            (
                spot.has(dr, 0),
                spot.has(-dr, 0),
                strip(ch, dr, (1, 2), TILE_ROWS[dr], FRAME_ROWS[dr], (1, 2), upright, k, spot.at(dr, 0)),
            )
            for k, dr in enumerate(SIDES)
        ])
        self.middle = both(lambda ch: [
            (
                spot.has(0, dc) & ~spot.far(dc),
                spot.has(0, -dc) & ~spot.far(-dc),
                strip(ch, 0, TILE_PLANES[dc], (H, F), (H, F), FRAME_PLANES[dc], level, n, spot.at(0, dc)),
            )
            for n, dc in enumerate(SIDES)
        ])
        self.corners = both(lambda ch: [
            (
                spot.has(side, 0) & spot.has(0, dc) & ~spot.far(dc),
                spot.has(side, 0) & spot.has(0, -dc) & ~spot.far(-dc),
                strip(ch, 0, TILE_PLANES[dc], OUTER_ROWS[side], OUTER_ROWS[side], FRAME_PLANES[dc], corner, 2 * k + n, spot.at(0, dc)),
            )
            for k, side in enumerate(SIDES)
            for n, dc in enumerate(SIDES)
        ])
        half = spot.half
        self.relays = [
            Relay(
                spot, dr, count,
                lambda row, dr=dr, count=count: frame.at[:, pl.ds(2 - half, 1), pl.ds(TILE_ROWS[dr][0] + row, count)],
                lambda row, dr=dr, count=count: frame.at[:, pl.ds(3 * half, 1), pl.ds(FRAME_ROWS[dr][0] + row, count)],
                held[i], relay_sems[2 * i], relay_sems[2 * i + 1],
            )
            for i, (dr, count) in enumerate(STRIPS)
        ]

    def begin(self, ch):
        self.vertical[ch].start()

    def aside(self):
        for relay in self.relays:
            relay.start()
        self.middle[0].start()
        self.middle[1].start()
        for relay in self.relays:
            relay.turn()

    def end(self):
        for ch in range(2):
            self.vertical[ch].wait_recv()
            self.corners[ch].start()
        for ch in range(2):
            self.middle[ch].wait_recv()
        for relay in self.relays:
            relay.wait_recv()
        for ch in range(2):
            self.corners[ch].wait_recv()
        for ch in range(2):
            for transfers in (self.vertical[ch], self.middle[ch], self.corners[ch]):
                transfers.wait_send()
        for relay in self.relays:
            relay.wait_send()


def pairs(sems):
    return [(sems[i], sems[i + 1]) for i in range(0, len(sems), 2)]


class Fold:
    def __init__(self, spot, accum, cbuf, mbuf, vbuf, fbuf, stack, held, upright, level, corner, *relay_sems):
        self.spot, self.accum, self.stack = spot, accum, stack
        self.cbuf, self.mbuf, self.vbuf, self.fbuf = cbuf, mbuf, vbuf, fbuf

        def strip(ch, planes, rows, buf, sems, k, device):
            return lambda: remote(accum.at[ch, part(planes), part(rows)], buf.at[ch, k], sems, (ch, k), device)

        def both(make):
            return [Transfers(make(ch)) for ch in range(2)]

        self.corners = both(lambda ch: [
            (
                spot.has(side, 0) & spot.has(0, dc) & ~spot.far(dc),
                spot.has(side, 0) & spot.has(0, -dc) & ~spot.far(-dc),
                strip(ch, OUTER_PLANES[dc], OUTER_ROWS[side], cbuf, corner, 2 * k + n, spot.at(0, dc)),
            )
            for k, side in enumerate(SIDES)
            for n, dc in enumerate(SIDES)
        ])
        self.middle = both(lambda ch: [
            (
                spot.has(0, dc) & ~spot.far(dc),
                spot.has(0, -dc) & ~spot.far(-dc),
                strip(ch, OUTER_PLANES[dc], (H, F), mbuf, level, n, spot.at(0, dc)),
            )
            for n, dc in enumerate(SIDES)
        ])
        self.vertical = both(lambda ch: [
            (
                spot.has(dr, 0),
                spot.has(-dr, 0),
                lambda k=k, dr=dr: remote(stack.at[ch, k], vbuf.at[ch, k], upright, (ch, k), spot.at(dr, 0)),
            )
            for k, dr in enumerate(SIDES)
        ])
        half = spot.half
        targets = {
            -1: lambda row, count: fbuf.at[:, 1 - half, :, pl.ds(row, count)],
            1: lambda row, count: fbuf.at[:, 3 - half, :, pl.ds(row, count)],
            0: lambda row, count: mbuf.at[:, 1 - half, :, pl.ds(row, count)],
        }
        self.relays = [
            Relay(
                spot, dr, count,
                lambda row, dr=dr, count=count: accum.at[:, pl.ds(3 - 3 * half, 1), pl.ds(OUTER_ROWS[dr][0] + row, count)],
                lambda row, dr=dr, count=count: targets[dr](row, count),
                held[i], relay_sems[2 * i], relay_sems[2 * i + 1],
            )
            for i, (dr, count) in enumerate(STRIPS)
        ]

    def begin(self):
        self.corners[0].start()
        self.corners[1].start()

    def aside(self):
        for relay in self.relays:
            relay.start()
        self.middle[0].start()
        self.middle[1].start()

    def pass_on(self):
        for relay in self.relays:
            relay.turn()

    def turn(self, ch):
        stack, cbuf = self.stack, self.cbuf
        for k, side in enumerate(SIDES):
            stack[ch, k] = self.accum[ch, 1:3, part(OUTER_ROWS[side])]
        self.corners[ch].wait_recv()
        for (_, received, _), (k, n) in zip(self.corners[ch].entries, FOUR):

            @pl.when(received)
            def _():
                plane = INNER_PLANES[SIDES[n]][0] - 1
                stack[ch, k, plane] = stack[ch, k, plane] + cbuf[ch, 2 * k + n, 0]

        self.vertical[ch].start()

    def end(self, ch, add):
        spot = self.spot
        self.middle[ch].wait_recv()
        if ch == 0:
            for relay in self.relays:
                relay.wait_recv()
        for n, dc in enumerate(SIDES):

            @pl.when(spot.has(0, -dc))
            def _():
                add(self.mbuf.at[ch, n], (H, F), INNER_PLANES[dc])

        self.vertical[ch].wait_recv()
        for k, dr in enumerate(SIDES):

            @pl.when(spot.has(-dr, 0))
            def _():
                add(self.vbuf.at[ch, k], INNER_ROWS[dr], (1, 2))

        for k, n in FOUR:
            dr, dc = SIDES[k], SIDES[n]

            @pl.when(spot.has(-dr, -dc) & spot.far(-dc))
            def _():
                add(self.fbuf.at[ch, 2 * k + n], INNER_ROWS[dr], INNER_PLANES[dc])

    def close(self):
        for ch in range(2):
            for transfers in (self.corners[ch], self.middle[ch], self.vertical[ch]):
                transfers.wait_send()
        for relay in self.relays:
            relay.wait_send()


def renew(spot, fold, halo, accum, frame, place_channel):
    for ch in range(2):
        place_channel(ch)
        fold.corners[ch].start()
    fold.aside()
    fold.turn(0)
    fold.turn(1)
    fold.pass_on()
    frame[:, 1:3, H : H + F] = frame[:, 1:3, H : H + F] + accum[:, 1:3, H : H + F]
    for ch in range(2):

        def add(buf, rows, planes):
            where = (ch, part(planes), part(rows))
            frame[where] = frame[where] + buf[...]

        fold.end(ch, add)
        halo.begin(ch)
    halo.aside()
    halo.end()
    fold.close()


def held_buffers():
    return [pltpu.VMEM((2, 1, count, H), jnp.float32) for _, count in STRIPS]


def fold_buffers():
    f32 = jnp.float32
    return [
        pltpu.VMEM((2, 4, 1, H, H), f32),
        pltpu.VMEM((2, 2, 1, F, H), f32),
        pltpu.VMEM((2, 2, 2, H, H), f32),
        pltpu.VMEM((2, 4, 1, H, H), f32),
        pltpu.VMEM((2, 2, 2, H, H), f32),
    ]


def exchange_sems():
    dma = pltpu.SemaphoreType.DMA
    shapes = ((2, 2), (2, 2), (2, 4)) + ((SEAM,),) * 6
    return [dma(shape) for shape in shapes for _ in range(2)]


CHUNK1 = 64
CHUNK2 = 16
COLORS = (("x", "y"), ("y", "x"))


def torus():
    sy, sx = lax.axis_index("sy"), lax.axis_index("sx")
    here = {
        "y": lax.div(sy, 4),
        "x": lax.div(lax.rem(sx, 8), 2),
        "z": lax.div(sx, 8) * 4 + lax.rem(sy, 4),
        "core": lax.rem(sx, 2),
    }
    size = {"x": 4, "y": 4, "z": 8, "core": 2}

    def place(axis, step):
        there = dict(here)
        there[axis] = lax.rem(here[axis] + step, size[axis])
        device = (
            there["y"] * 4 + lax.rem(there["z"], 4),
            lax.div(there["z"], 4) * 8 + there["x"] * 2 + there["core"],
        )
        return there[axis], device

    return here, place


def finish_all(fold, place_channel, accum, old, g, probe_re, probe_im, out_re, out_im, out, *rest):
    r0, w0, r1, w1, r2, w2, r3, w4, s0, q0, s1, q1, s2, q2, s3, q3, s4, q4, s5, q5, s6, q6 = rest
    here, place = torus()
    rate = PROBE_GAIN / (8 * math.sqrt(ROWS * COLS))
    core = here["core"]
    other, partner = place("core", 1)
    mine = pl.ds(pl.multiple_of(core * 512, 512), 512)
    theirs = pl.ds(pl.multiple_of(other * 512, 512), 512)

    def send(src, dst, ss, rs, device):
        copy = pltpu.make_async_remote_copy(
            src_ref=src, dst_ref=dst, send_sem=ss, recv_sem=rs, device_id=device, device_id_type=MESH
        )
        copy.start()
        return copy

    def rows(start, count):
        return pl.ds(pl.multiple_of(start, count), count)

    def wait(copies):
        for copy in copies:
            copy.wait()

    across_cores = send(g.at[theirs], r0, s0, q0, partner)
    place_channel(0)
    place_channel(1)
    across_cores.wait()
    w0[...] = g[mine] + r0[...]

    copies = []
    for c, (first, second) in enumerate(COLORS):
        copies.append([])
        for step in (1, 2, 3):
            index, device = place(first, step)
            source = w0.at[rows(c * 256 + index * CHUNK1, CHUNK1)]
            copies[c].append(send(source, r1.at[c, step - 1], s1.at[c, step - 1], q1.at[c, step - 1], device))
    fold.begin()
    for c, (first, second) in enumerate(COLORS):
        wait(copies[c])
        own = w0[rows(c * 256 + here[first] * CHUNK1, CHUNK1)]
        w1[c] = (own + r1[c, 0]) + (r1[c, 1] + r1[c, 2])
        copies[c] = []
        for step in (1, 2, 3):
            index, device = place(second, step)
            source = w1.at[c, rows(index * CHUNK2, CHUNK2)]
            copies[c].append(send(source, r2.at[c, step - 1], s2.at[c, step - 1], q2.at[c, step - 1], device))
    fold.turn(0)
    for c, (first, second) in enumerate(COLORS):
        wait(copies[c])
        own = w1[c, rows(here[second] * CHUNK2, CHUNK2)]
        w2[c] = (own + r2[c, 0]) + (r2[c, 1] + r2[c, 2])
        copies[c] = []
        for step in range(1, 8):
            device = place("z", step)[1]
            copies[c].append(send(w2.at[c], r3.at[c, here["z"]], s3.at[c, step - 1], q3.at[c, step - 1], device))
        r3[c, here["z"]] = w2[c]
    fold.turn(1)
    fold.aside()
    fold.pass_on()
    outs = (out_re, out_im)
    for channel, tile in enumerate(outs):
        for n in range(2):
            tile[:, n * H : (n + 1) * H] = old[channel, 1 + n, H : H + F] + accum[channel, 1 + n, H : H + F]
    for c, (first, second) in enumerate(COLORS):
        wait(copies[c])
        total = ((r3[c, 0] + r3[c, 1]) + (r3[c, 2] + r3[c, 3])) + ((r3[c, 4] + r3[c, 5]) + (r3[c, 6] + r3[c, 7]))
        start = c * 256 + here[first] * CHUNK1 + here[second] * CHUNK2
        own = rows(lax.rem(start, F), CHUNK2)
        mode = lax.div(start, F)
        base = jnp.where(core == 0, probe_re[mode, own], probe_im[mode, own])
        spot = rows(here[second] * CHUNK2, CHUNK2)
        w4[c, spot] = base + rate * total
        copies[c] = []
        for step in (1, 2, 3):
            device = place(second, step)[1]
            copies[c].append(send(w4.at[c, spot], w4.at[c, spot], s4.at[c, step - 1], q4.at[c, step - 1], device))
    last = []
    for c, (first, second) in enumerate(COLORS):
        wait(copies[c])
        spot = out.at[rows(core * 512 + c * 256 + here[first] * CHUNK1, CHUNK1)]
        copies[c] = []
        for step in (1, 2, 3):
            device = place(first, step)[1]
            copies[c].append(send(w4.at[c], spot, s5.at[c, step - 1], q5.at[c, step - 1], device))
        out[rows(core * 512 + c * 256 + here[first] * CHUNK1, CHUNK1)] = w4[c]
        last.append(send(w4.at[c], spot, s6.at[c, 0], q6.at[c, 0], partner))
    for ch, tile in enumerate(outs):

        def add(buf, where_rows, planes):
            for n in range(planes[1]):
                where = (pl.ds(where_rows[0] - H, where_rows[1]), pl.ds((planes[0] - 1 + n) * H, H))
                tile[where] = tile[where] + buf[n]

        fold.end(ch, add)
    for c, (first, second) in enumerate(COLORS):
        for step in (1, 2, 3):
            copies[c][step - 1].wait()
            source = place(first, 4 - step)[0]
            spot = out.at[rows(core * 512 + c * 256 + source * CHUNK1, CHUNK1)]
            last.append(send(spot, spot, s6.at[c, step], q6.at[c, step], partner))
    fold.close()
    wait(last)


def write_kernel(a, b, flat, out_a, out_b, out_c, out_d, held_a, held_b, held_flat, load_sem, store_sem):
    parts = [(a, held_a, out_a), (b, held_b, out_b)]
    for k, out in enumerate((out_c, out_d)):
        for m in range(2):
            rows = pl.ds((2 * k + m) * F, F)
            parts.append((flat.at[rows], held_flat.at[rows], out.at[m]))
    loads = [pltpu.make_async_copy(src, held, load_sem.at[i]) for i, (src, held, _) in enumerate(parts)]
    stores = [pltpu.make_async_copy(held, out, store_sem.at[i]) for i, (_, held, out) in enumerate(parts)]
    for load in loads:
        load.start()
    for load, store in zip(loads, stores):
        load.wait()
        store.start()
    for store in stores:
        store.wait()


def place_terms(ch, batch, order, offsets, accum, padded):
    starts = []
    for j in range(4):
        starts.append(F - (offsets[0, 0, 0, order[0, 0, batch * 4 + j]] + H))
    for n in range(4):
        for row in range(0, E, H):
            parts = [padded[j, ch, n, pl.ds(starts[j] + row, H), :] for j in range(4)]
            accum[ch, n, row : row + H, :] = (parts[0] + parts[1]) + (parts[2] + parts[3])


def work(batch, order, offsets, frame, probe_re, probe_im, amps, amp_ready, left, right, accum, grad, scale, padded, patch, fields, halves):
    back_left, back_right = right, left
    size = 4
    for j in range(size):
        p = order[0, 0, batch * size + j]
        top = offsets[0, 0, 0, p] + H
        shift = offsets[0, 0, 1, p] + H
        for ch in range(2):
            rows = jnp.concatenate([frame[ch, n, pl.ds(top, F), :] for n in range(4)], axis=1)
            patch[j, ch] = pltpu.roll(rows, lax.rem(E - shift, E), 1)[:, :F]
        re, im = patch[j, 0], patch[j, 1]
        for m in range(2):
            at = pl.ds((2 * j + m) * F, F)
            fields[0:F, at] = (probe_re[m] * re - probe_im[m] * im).astype(jnp.bfloat16)
            fields[F : 2 * F, at] = (probe_re[m] * im + probe_im[m] * re).astype(jnp.bfloat16)
    for n in range(2 * size):
        half = jnp.dot(left[...], fields[0 : 2 * F, n * F : (n + 1) * F], preferred_element_type=jnp.float32)
        halves[n * F : (n + 1) * F, 0:F] = half[0:F].astype(jnp.bfloat16)
        halves[n * F : (n + 1) * F, F : 2 * F] = half[F:].astype(jnp.bfloat16)
    for j in range(size):
        far = jnp.dot(halves[2 * j * F : 2 * (j + 1) * F, :], right[...], preferred_element_type=jnp.float32)
        squares = far * far
        intensity = (squares[0:F, 0:F] + squares[0:F, F:]) + (squares[F:, 0:F] + squares[F:, F:])
        if j == 0:
            amp_ready()
        ratio = amps[order[0, 0, batch * size + j]] * lax.rsqrt(jnp.maximum(intensity, 1.0))
        for m in range(2):
            at = (2 * j + m) * F
            fields[2 * F : 3 * F, at : at + F] = (far[m * F : (m + 1) * F, 0:F] * ratio).astype(jnp.bfloat16)
            fields[3 * F : 4 * F, at : at + F] = (far[m * F : (m + 1) * F, F:] * ratio).astype(jnp.bfloat16)
    for n in range(2 * size):
        half = jnp.dot(back_left[...], fields[2 * F :, n * F : (n + 1) * F], preferred_element_type=jnp.float32)
        halves[n * F : (n + 1) * F, 0:F] = half[0:F].astype(jnp.bfloat16)
        halves[n * F : (n + 1) * F, F : 2 * F] = half[F:].astype(jnp.bfloat16)
    for j in range(size):
        p = order[0, 0, batch * size + j]
        top = offsets[0, 0, 0, p] + H
        shift = offsets[0, 0, 1, p] + H
        back = jnp.dot(halves[2 * j * F : 2 * (j + 1) * F, :], back_right[...], preferred_element_type=jnp.float32)
        re, im = patch[j, 0], patch[j, 1]
        terms = [None, None]
        for m in range(2):
            at = (2 * j + m) * F
            d_re = back[m * F : (m + 1) * F, 0:F] - fields[0:F, at : at + F].astype(jnp.float32)
            d_im = back[m * F : (m + 1) * F, F:] - fields[F : 2 * F, at : at + F].astype(jnp.float32)
            o_re = probe_re[m] * d_re + probe_im[m] * d_im
            o_im = probe_re[m] * d_im - probe_im[m] * d_re
            g_re = re * d_re + im * d_im
            g_im = re * d_im - im * d_re
            if m == 0:
                terms = [o_re, o_im]
            else:
                terms = [terms[0] + o_re, terms[1] + o_im]
            for ch, g in enumerate((g_re, g_im)):
                own = pl.ds((2 * ch + m) * F, F)
                if j == 0 and batch == 0:
                    grad[own] = g
                else:
                    grad[own] = grad[own] + g
        for ch in range(2):
            wide = jnp.concatenate([terms[ch] * scale[0:1, 0:1], jnp.zeros((F, F), jnp.float32)], axis=1)
            wide = pltpu.roll(wide, shift, 1)
            for n in range(4):
                padded[j, ch, n, F : 2 * F, :] = wide[:, n * H : (n + 1) * H]


def whole_kernel(order, offsets, re_ref, im_ref, probe_re_in, probe_im_in, amps_in, left_in, right_in, out_re, out_im, out, *scratch):
    frame, accum, probe_re, probe_im, amps, left, right, grad, scale, padded, patch, fields, halves, load_sem = scratch[:14]
    buffers, held, sems, rest = scratch[14:24], scratch[24:36], pairs(scratch[36:108]), scratch[108:]
    spot = Spot()
    loads = [
        pltpu.make_async_copy(source, target, load_sem.at[i])
        for i, (source, target) in enumerate(
            [(probe_re_in, probe_re), (probe_im_in, probe_im), (left_in, left), (right_in, right), (amps_in, amps)]
        )
    ]
    for load in loads:
        load.start()

    def meanwhile():
        for channel, source in enumerate((re_ref, im_ref)):
            for n in range(2):
                frame[channel, 1 + n, H : H + F] = source[:, n * H : (n + 1) * H]
        clear_edges(spot.row, spot.col, frame)

    here, place = torus()
    yes = spot.row >= 0
    size = {"core": 2, "x": 4, "y": 4, "z": 8}
    greet(
        spot.peers()
        + [(yes, place(axis, step)[1]) for axis in size for step in range(1, size[axis])],
        meanwhile,
    )
    halo = Halo(spot, frame, held[0:3], *sems[0:9])
    halo.begin(0)
    halo.begin(1)
    halo.aside()
    blank = jnp.zeros((F, H), jnp.float32)
    for j in range(4):
        for ch in range(2):
            for n in range(4):
                padded[j, ch, n, 0:F] = blank
                padded[j, ch, n, 2 * F : 3 * F] = blank
    for load in loads[:4]:
        load.wait()
    power = jnp.max(
        probe_re[0] * probe_re[0]
        + probe_im[0] * probe_im[0]
        + (probe_re[1] * probe_re[1] + probe_im[1] * probe_im[1]),
        keepdims=True,
    )
    scale[...] = jnp.broadcast_to(OBJECT_RATE / power, (8, H))
    halo.end()
    common = (left, right, accum, grad, scale, padded, patch, fields, halves)
    work(0, order, offsets, frame, probe_re, probe_im, amps, loads[4].wait, *common)
    fold = Fold(spot, accum, *buffers[0:5], held[3:6], *sems[9:18])
    halo = Halo(spot, frame, held[6:9], *sems[18:27])
    renew(spot, fold, halo, accum, frame, lambda ch: place_terms(ch, 0, order, offsets, accum, padded))
    work(1, order, offsets, frame, probe_re, probe_im, amps, lambda: None, *common)
    fold = Fold(spot, accum, *buffers[5:10], held[9:12], *sems[27:36])
    finish_all(fold, lambda ch: place_terms(ch, 1, order, offsets, accum, padded), accum, frame, grad, probe_re, probe_im, out_re, out_im, out, *rest)


def local(object_re, object_im, probe_re, probe_im, amplitudes, offsets, visit_order):
    f32, bf16 = jnp.float32, jnp.bfloat16
    left, right = dft_operands()
    dma = pltpu.SemaphoreType.DMA
    tile_shape = jax.ShapeDtypeStruct((F, F), f32)
    out_re, out_im, flat = pl.pallas_call(
        whole_kernel,
        out_shape=[tile_shape, tile_shape, jax.ShapeDtypeStruct((4 * F, F), f32)],
        in_specs=[SMEM, SMEM, VMEM, VMEM, ANY, ANY, ANY, ANY, ANY],
        out_specs=[VMEM] * 3,
        scratch_shapes=[
            pltpu.VMEM((2, 4, E, H), f32),
            pltpu.VMEM((2, 4, E, H), f32),
            pltpu.VMEM((2, F, F), f32),
            pltpu.VMEM((2, F, F), f32),
            pltpu.VMEM((8, F, F), f32),
            pltpu.VMEM((2 * F, 2 * F), bf16),
            pltpu.VMEM((2 * F, 2 * F), bf16),
            pltpu.VMEM((4 * F, F), f32),
            pltpu.VMEM((8, H), f32),
            pltpu.VMEM((4, 2, 4, 3 * F, H), f32),
            pltpu.VMEM((4, 2, F, F), f32),
            pltpu.VMEM((4 * F, 8 * F), bf16),
            pltpu.VMEM((8 * F, 2 * F), bf16),
            dma((5,)),
        ]
        + fold_buffers()
        + fold_buffers()
        + held_buffers() * 4
        + exchange_sems() * 4
        + [
            pltpu.VMEM((512, F), f32),
            pltpu.VMEM((512, F), f32),
            pltpu.VMEM((2, 3, CHUNK1, F), f32),
            pltpu.VMEM((2, CHUNK1, F), f32),
            pltpu.VMEM((2, 3, CHUNK2, F), f32),
            pltpu.VMEM((2, CHUNK2, F), f32),
            pltpu.VMEM((2, 8, CHUNK2, F), f32),
            pltpu.VMEM((2, CHUNK1, F), f32),
            dma, dma,
            dma((2, 3)), dma((2, 3)),
            dma((2, 3)), dma((2, 3)),
            dma((2, 7)), dma((2, 7)),
            dma((2, 3)), dma((2, 3)),
            dma((2, 3)), dma((2, 3)),
            dma((2, 4)), dma((2, 4)),
        ],
        compiler_params=pltpu.CompilerParams(
            collective_id=0, has_side_effects=True, vmem_limit_bytes=62 * 1024 * 1024
        ),
    )(
        visit_order,
        jnp.swapaxes(offsets, 2, 3),
        object_re,
        object_im,
        probe_re,
        probe_im,
        amplitudes.reshape(8, F, F),
        left,
        right,
    )
    probe_shape = jax.ShapeDtypeStruct((2, F, F), f32)
    return tuple(
        pl.pallas_call(
            write_kernel,
            out_shape=[tile_shape, tile_shape, probe_shape, probe_shape],
            in_specs=[ANY] * 3,
            out_specs=[ANY] * 4,
            scratch_shapes=[
                pltpu.VMEM((F, F), f32),
                pltpu.VMEM((F, F), f32),
                pltpu.VMEM((4 * F, F), f32),
                dma((6,)),
                dma((6,)),
            ],
        )(out_re, out_im, flat)
    )


def solution(mesh):
    return jax.shard_map(
        local,
        mesh=mesh,
        in_specs=(
            P("sy", "sx"),
            P("sy", "sx"),
            P(),
            P(),
            P("sy", "sx", None, None, None),
            P("sy", "sx", None, None),
            P("sy", "sx", None),
        ),
        out_specs=(P("sy", "sx"), P("sy", "sx"), P(), P()),
        check_vma=False,
    )
```
